32 devices in a mesh: tm: 4 (over y, x), chan: 8 (over z, core).
Axes of the slice: x: 2, y: 2, z: 4, core: 2. Of those that a mesh axis runs over, the one named last changes fastest.
Arguments:
- voltages: bfloat16 [8, 4, 32768, 512], P(None, None, ('tm', 'chan')), may hold values from -6 to 6
- taps: float32 [4, 512], replicated, may hold values from -3 to 3
- busy_mask: int32 [512], replicated, may hold values from 0 to 1, as said below
- drift_low: int32 [512], replicated, may hold values from -16 to 1
Outputs:
- drift_power: float32 [8, 32, 16, 2048], P(None, 'chan', None, 'tm')
The draws below stay inside these ranges and needn't reach their ends.
Inputs may be any that keep to these rules, and one draw needn't show every extreme that they name: `busy_mask`: exactly 32 entries are 1.
All inputs are finite; a program needn't handle non-finite values.
Results may differ from the reference program's by a relative error of at most 0.008.
Values may be sent and summed in bfloat16 or wider, within the bound.
A program may use at most 192 MiB of HBM per device.

```python
import math
import jax
import jax.numpy as jnp
from jax import lax

COARSE_CHANNELS = 512
FINE = 2048
FA = 32
FB = 64
TAPS = 4
NDRIFT = 16
DSPAN = 16
FSTEP = 4
BEAMS = 8
SPEC = 32768
STEPS = 16
BUSY = 32
N_TM = 4


def draw_busy_mask(key, part):
    perm_key = jax.random.fold_in(key, 11)
    reward_key = jax.random.fold_in(key, 23)
    permuted_order = jax.random.permutation(perm_key, COARSE_CHANNELS).astype(jnp.int32)
    block_reward = jax.random.randint(reward_key, (COARSE_CHANNELS // 8,), 0, 4, dtype=jnp.int32)
    merit_scores = jnp.repeat(block_reward, 8, total_repeat_length=COARSE_CHANNELS) * (2 * COARSE_CHANNELS) + permuted_order
    chosen = lax.top_k(merit_scores, BUSY)[1]
    return jnp.zeros((COARSE_CHANNELS,), jnp.int32).at[chosen].set(1)


def set_ends(drawn, key, low, largest):
    longest = drawn.shape.index(max(drawn.shape))
    spots = []
    for shift in (0, 1):
        where = [jax.random.randint(jax.random.fold_in(key, axis), (), 0, length) for axis, length in enumerate(drawn.shape)]
        where[longest] = (where[longest] + shift) % drawn.shape[longest]
        spots.append(tuple(where))
    return drawn.at[spots[0]].set(low).at[spots[1]].set(largest)


def levels(own_key, extent, cuts, least, high):
    def one(axis_at, shards_of):
        draws = jax.random.uniform(jax.random.fold_in(jax.random.fold_in(own_key, 6), axis_at), (shards_of,), jnp.float32, least / len(cuts), high / len(cuts))
        return jnp.repeat(jnp.exp(draws), extent[axis_at] // shards_of).reshape((-1,) + (1,) * (len(extent) - axis_at - 1))

    factor_of = one(*cuts[0])
    for cut in cuts[1:]:
        factor_of = factor_of * one(*cut)
    return factor_of


def noise(key, dims, spread, most, shards=(), kind=jnp.bfloat16):
    level = levels(key, dims, shards, -0.22, 0.18) if shards else 1.0
    values = jax.random.normal(key, dims, jnp.float32) * spread * level
    return jnp.minimum(jnp.maximum(values, -most), most).astype(kind)


def setup_inputs(seed: int = 0) -> dict:
    keys = jax.random.split(jax.random.key(seed), 5)
    return {
        "voltages": noise(keys[0], (BEAMS, 4, SPEC, COARSE_CHANNELS), 1.0, 6.0, ((2, 32),)),
        "taps": noise(keys[1], (TAPS, COARSE_CHANNELS), 0.5, 3.0, (), jnp.float32),
        "busy_mask": draw_busy_mask(jax.random.fold_in(keys[4], 71), 0),
        "drift_low": set_ends(jax.random.randint(keys[3], (COARSE_CHANNELS,), -DSPAN, DSPAN - NDRIFT + 2), jax.random.fold_in(keys[3], 1), -DSPAN, (DSPAN - NDRIFT + 2) - 1).astype(jnp.int32),
    }


def busy_index(busy_mask, busy_count):
    mask_ints = busy_mask.astype(jnp.int32)
    before = (jnp.cumsum(mask_ints) - mask_ints).astype(jnp.int32)
    slot_ids = jnp.arange(busy_count, dtype=jnp.int32)
    is_slot = (mask_ints[:, None] == 1) & (before[:, None] == slot_ids[None, :])
    positions = jnp.arange(busy_mask.shape[0], dtype=jnp.int32)
    return jnp.sum(jnp.where(is_slot, positions[:, None], 0), axis=0).astype(jnp.int32)


def real_dft(sample_pos, freq_ids, length):
    phase_index = (sample_pos[:, None] * freq_ids[None, :]) % length
    angles = phase_index.astype(jnp.float32) * (2.0 * math.pi / length)
    cosines = jnp.cos(angles)
    sine_table = jnp.sin(angles)
    upper = jnp.stack([cosines, -sine_table], axis=1)
    lower = jnp.stack([sine_table, cosines], axis=1)
    return jnp.stack([upper, lower], axis=0).astype(jnp.bfloat16)


def to_bfloat(values):
    return lax.optimization_barrier(values.astype(jnp.bfloat16)).astype(jnp.float32)


def detect_power(spectra):
    items, lanes, chan_rows, samples = spectra.shape
    step_count = samples // (FA * FB)
    shaped = spectra.reshape(items, 2, 2, chan_rows, step_count, FA, FB).astype(jnp.float32)
    short_ids = jnp.arange(FA, dtype=jnp.int32)
    long_ids = jnp.arange(FB, dtype=jnp.int32)
    first_dft = real_dft(short_ids, short_ids, FA).astype(jnp.float32)
    second_dft = real_dft(long_ids, long_ids, FB).astype(jnp.float32)
    first_pass = jnp.einsum("xopctab,paqf->xoqctfb", shaped, first_dft, precision=lax.Precision.HIGHEST)
    twist = (short_ids[:, None] * long_ids[None, :]) % (FA * FB)
    twist_angles = twist.astype(jnp.float32) * (2.0 * math.pi / (FA * FB))
    twist_cos = jnp.cos(twist_angles)
    twist_sin = jnp.sin(twist_angles)
    real_part = first_pass[:, :, 0]
    imag_part = first_pass[:, :, 1]
    turned = jnp.stack([real_part * twist_cos + imag_part * twist_sin, imag_part * twist_cos - real_part * twist_sin], axis=2).astype(jnp.bfloat16)
    second_pass = jnp.einsum("xoqctfb,qbsg->xosctgf", turned.astype(jnp.float32), second_dft, precision=lax.Precision.HIGHEST)
    powers = jnp.sum(second_pass * second_pass, axis=(1, 2)) / (4.0 * FA * FB)
    return powers.reshape(items, chan_rows, step_count, FA * FB)


def drift_rows(step_rows, first_step, drift_rates, first_bin, bin_width, pad_width):
    padded = jnp.pad(step_rows, ((0, 0), (0, 0), (0, 0), (pad_width, pad_width)))
    chan_rows = step_rows.shape[1]
    chan_pick = jnp.arange(chan_rows, dtype=jnp.int32)[:, None, None]
    start_offsets = jnp.arange(bin_width, dtype=jnp.int32)
    running = jnp.zeros((step_rows.shape[0], chan_rows, drift_rates.shape[1], bin_width), jnp.float32)
    for row_index in range(step_rows.shape[2]):
        step_time = first_step + row_index
        anchor = pad_width + first_bin + drift_rates * step_time
        positions = (anchor[:, :, None] + start_offsets[None, None, :]).astype(jnp.int32)
        picked = padded[:, :, row_index][:, chan_pick, positions]
        running = running + picked
    return running


def reference(voltages, taps, busy_mask, drift_low):
    slot_index = busy_index(busy_mask, BUSY)
    coarse_dft = real_dft(jnp.arange(COARSE_CHANNELS, dtype=jnp.int32), slot_index, COARSE_CHANNELS).astype(jnp.float32)

    def one_beam(beam_volts):
        extended = jnp.pad(beam_volts, ((0, 0), (0, TAPS - 1), (0, 0)))
        filtered = taps[0] * extended[:, 0:SPEC]
        for tap_index in range(1, TAPS):
            filtered = filtered + taps[tap_index] * extended[:, tap_index:tap_index + SPEC]
        filtered = filtered.astype(jnp.bfloat16).astype(jnp.float32).reshape(2, 2, SPEC, COARSE_CHANNELS)
        coarse = jnp.einsum("opsn,pnqr->oqrs", filtered, coarse_dft, precision=lax.Precision.HIGHEST)
        coarse = (coarse * COARSE_CHANNELS ** -0.5).astype(jnp.bfloat16)
        return detect_power(coarse.reshape(1, 4, BUSY, SPEC))[0]

    powers = lax.map(one_beam, voltages)
    low_rates = drift_low[slot_index].astype(jnp.int32)
    drift_rates = (low_rates[:, None] + jnp.arange(NDRIFT, dtype=jnp.int32)[None, :]).astype(jnp.int32)
    pad_width = DSPAN * (STEPS - 1)
    drift_total = jnp.zeros((BEAMS, BUSY, NDRIFT, FINE), jnp.float32)
    for group_index in range(N_TM):
        step_rows = powers[:, :, group_index * FSTEP:(group_index + 1) * FSTEP]
        drift_total = drift_total + to_bfloat(drift_rows(step_rows, group_index * FSTEP, drift_rates, 0, FINE, pad_width))
    return drift_total / STEPS
```

```python
import math

import jax
import jax.numpy as jnp
import numpy as np
from jax import lax
from jax.experimental import pallas as pl
from jax.experimental.pallas import tpu as pltpu
from jax.sharding import PartitionSpec as P

FA = 32
FB = 64
TAPS = 4
NDRIFT = 16
DSPAN = 16
FSTEP = 4
CH_DEV = 1


def passed_along(block, axis, distance):
    devices = range(lax.axis_size(axis))
    route = [(i - distance, i) for i in devices if i - distance in devices]
    return lax.ppermute(block, axis, route)


def busy_index(busy_mask, busy_count):
    before = jnp.cumsum(busy_mask) - busy_mask
    slot_ids = jnp.arange(busy_count, dtype=jnp.int32)
    is_slot = (busy_mask[:, None] == 1) & (before[:, None] == slot_ids[None, :])
    positions = jnp.arange(busy_mask.shape[0], dtype=jnp.int32)
    return jnp.sum(jnp.where(is_slot, positions[:, None], 0), axis=0)


def real_dft(sample_pos, freq_ids, length):
    phase_index = sample_pos[:, None] * freq_ids[None, :] % length
    angles = phase_index.astype(jnp.float32) * (2.0 * math.pi / length)
    cosines = jnp.cos(angles)
    sine_table = jnp.sin(angles)
    upper = jnp.stack([cosines, -sine_table], axis=1)
    lower = jnp.stack([sine_table, cosines], axis=1)
    return jnp.stack([upper, lower], axis=0).astype(jnp.bfloat16)


def to_bfloat(values):
    return lax.optimization_barrier(values.astype(jnp.bfloat16)).astype(jnp.float32)


def detect_power(spectra):
    items, lanes, chan_rows, samples = spectra.shape
    step_count = samples // (FA * FB)
    shaped = spectra.reshape(items, 2, 2, chan_rows, step_count, FA, FB)
    short_ids = jnp.arange(FA, dtype=jnp.int32)
    long_ids = jnp.arange(FB, dtype=jnp.int32)
    first_pass = jnp.einsum(
        "xopctab,paqf->xoqctfb",
        shaped,
        real_dft(short_ids, short_ids, FA),
        preferred_element_type=jnp.float32,
    )
    twist = short_ids[:, None] * long_ids[None, :] % (FA * FB)
    twist_angles = twist.astype(jnp.float32) * (2.0 * math.pi / (FA * FB))
    twist_cos = jnp.cos(twist_angles)
    twist_sin = jnp.sin(twist_angles)
    real_part = first_pass[:, :, 0]
    imag_part = first_pass[:, :, 1]
    turned = jnp.stack(
        [
            real_part * twist_cos + imag_part * twist_sin,
            imag_part * twist_cos - real_part * twist_sin,
        ],
        axis=2,
    ).astype(jnp.bfloat16)
    second_pass = jnp.einsum(
        "xoqctfb,qbsg->xosctgf",
        turned,
        real_dft(long_ids, long_ids, FB),
        preferred_element_type=jnp.float32,
    )
    powers = jnp.sum(second_pass * second_pass, axis=(1, 2)) / (4.0 * FA * FB)
    return powers.reshape(items, chan_rows, step_count, FA * FB)


def drift_rows(step_rows, first_step, drift_rates, first_bin, bin_width, pad_width):
    padded = jnp.pad(step_rows, ((0, 0), (0, 0), (0, 0), (pad_width, pad_width)))
    chan_rows = step_rows.shape[1]
    rate_count = drift_rates.shape[1]
    running = jnp.zeros((step_rows.shape[0], chan_rows, rate_count, bin_width), jnp.float32)
    for row_index in range(step_rows.shape[2]):
        step_time = first_step + row_index
        power_row = padded[:, 0, row_index]
        windows = []
        for rate_pos in range(rate_count):
            start = pad_width + first_bin + drift_rates[0, rate_pos] * step_time
            windows.append(lax.dynamic_slice_in_dim(power_row, start, bin_width, 1))
        per_slot = [jnp.stack(windows, axis=1)]
        running = running + jnp.stack(per_slot, axis=1)
    return running


def slot_rates(slot_part, drift_low):
    one_hot = slot_part[:, None] == jnp.arange(drift_low.shape[0], dtype=jnp.int32)[None, :]
    low_rates = jnp.sum(jnp.where(one_hot, drift_low[None, :], 0), axis=1)
    return low_rates[:, None] + jnp.arange(NDRIFT, dtype=jnp.int32)[None, :]


def shards(voltages, taps, busy_mask, drift_low):
    tm_count = lax.axis_size("tm")
    chan_devices = lax.axis_size("chan")
    count_of_beams, lanes, spec_dev, chan_count = voltages.shape
    busy_count = CH_DEV * tm_count * chan_devices
    step_count = FSTEP * tm_count
    pad_width = DSPAN * (step_count - 1)
    slot_index = busy_index(busy_mask, busy_count)
    slot_order = (
        slot_index.reshape(chan_devices, tm_count, CH_DEV).transpose(1, 0, 2).reshape(busy_count)
    )
    coarse_dft = real_dft(jnp.arange(chan_count, dtype=jnp.int32), slot_order, chan_count)
    following = passed_along(voltages[:, :, : TAPS - 1], ("tm", "chan"), -1)
    extended = jnp.concatenate([voltages, following], axis=2)
    filtered = taps[0] * extended[:, :, 0:spec_dev]
    for tap_index in range(1, TAPS):
        filtered = filtered + taps[tap_index] * extended[:, :, tap_index : tap_index + spec_dev]
    filtered = filtered.astype(jnp.bfloat16).reshape(count_of_beams, 2, 2, spec_dev, chan_count)
    coarse = jnp.einsum(
        "bopsn,pnqr->boqrs", filtered, coarse_dft, preferred_element_type=jnp.float32
    )
    coarse = (
        (coarse * chan_count ** (-0.5))
        .astype(jnp.bfloat16)
        .reshape(count_of_beams, 4, busy_count, spec_dev)
    )
    arrived = lax.all_to_all(
        lax.all_to_all(coarse, "tm", split_axis=2, concat_axis=3, tiled=True),
        "chan",
        split_axis=2,
        concat_axis=3,
        tiled=True,
    )
    ordered = arrived.reshape(count_of_beams, 4, CH_DEV, chan_devices, tm_count, spec_dev)
    ordered = ordered.transpose(0, 1, 2, 4, 3, 5).reshape(
        count_of_beams, 4, CH_DEV, tm_count * chan_devices * spec_dev
    )
    powers = detect_power(ordered)
    first_slot = lax.axis_index("chan") * (CH_DEV * tm_count) + lax.axis_index("tm") * CH_DEV
    drift_rates = slot_rates(lax.dynamic_slice_in_dim(slot_index, first_slot, CH_DEV), drift_low)
    drift_total = jnp.zeros((count_of_beams, CH_DEV, NDRIFT, FA * FB), jnp.float32)
    for group_index in range(tm_count):
        step_rows = powers[:, :, group_index * FSTEP : (group_index + 1) * FSTEP]
        drift_total = drift_total + to_bfloat(
            drift_rows(step_rows, group_index * FSTEP, drift_rates, 0, FA * FB, pad_width)
        )
    result = lax.all_to_all(
        (drift_total / step_count).astype(jnp.bfloat16),
        "tm",
        split_axis=3,
        concat_axis=1,
        tiled=True,
    ).astype(jnp.float32)
    return result


LANES = 128
FINE = FA * FB
SHORT = FINE // LANES
SLOTS = 32
HALO_ROWS = 8
PAD = 256
BLOCK = 256
DEPTH = 3


def short_dft(values, sign):
    count = len(values)
    if count == 1:
        return values
    even = short_dft(values[0::2], sign)
    odd = short_dft(values[1::2], sign)
    low, high = [], []
    for k in range(count // 2):
        term = odd[k]
        if k:
            flipped = pltpu.roll(term, LANES // 2, 1)
            angle = 2.0 * math.pi * k / count
            if 4 * k == count:
                term = flipped * sign
            else:
                term = term * math.cos(angle) + flipped * (sign * math.sin(angle))
        low.append(even[k] + term)
        high.append(even[k] - term)
    return low + high


def first_block(part):
    return jnp.clip(2 * part - 1, 0, (FINE - 2 * PAD) // BLOCK - 2)


def front_kernel(
    tm_count, chan_devices, volt, taps_ref, mask_ref, rate_ref, trig_hbm, dft_hbm, tap_ref, pick_ref,
    out_ref, low_ref, vbuf, halo, trig, dft, weight, edge, g00, g01, g10, g11, spec, mid, power, send, held,
    volt_sem, const_sem, halo_sem, swap_sent, swap_came, sent1, came1, sent2, came2,
):
    beams, lanes, rows, chan_count = volt.shape
    items = beams // 2
    count = rows // SHORT
    tm, chan = lax.axis_index("tm"), lax.axis_index("chan")
    core = lax.rem(chan, 2)
    place = tm * chan_devices + chan
    last_place = tm_count * chan_devices - 1
    MESH = pl.DeviceIdType.MESH
    tm_peers = [lax.rem(tm + q, tm_count) for q in range(tm_count)]
    chan_peers = [lax.rem(chan + k, chan_devices) for k in range(chan_devices)]
    chan_from = [lax.rem(chan + chan_devices - k, chan_devices) for k in range(chan_devices)]
    tm_from = [lax.rem(tm + tm_count - q, tm_count) for q in range(tm_count)]
    before = lax.rem(place + last_place, last_place + 1)
    after = lax.rem(place + 1, last_place + 1)
    before_id = (before // chan_devices, lax.rem(before, chan_devices))
    after_id = (after // chan_devices, lax.rem(after, chan_devices))

    barrier = pltpu.get_barrier_semaphore()
    for q in range(1, tm_count):
        pl.semaphore_signal(barrier, inc=1, device_id=(tm_peers[q], chan), device_id_type=MESH)
    for k in range(1, chan_devices):
        pl.semaphore_signal(barrier, inc=1, device_id=(tm, chan_peers[k]), device_id_type=MESH)
    pl.semaphore_signal(barrier, inc=1, device_id=before_id, device_id_type=MESH)
    pl.semaphore_signal(barrier, inc=1, device_id=after_id, device_id_type=MESH)

    def volt_copy(i):
        beam = lax.rem(core + 1 + i, 2) * items + i // 2
        slot = lax.rem(i, DEPTH)
        return pltpu.make_async_copy(volt.at[beam], vbuf.at[slot], volt_sem.at[slot])

    trig_copy = pltpu.make_async_copy(trig_hbm, trig, const_sem.at[0])
    dft_copy = pltpu.make_async_copy(dft_hbm, dft, const_sem.at[1])
    trig_copy.start()
    volt_copy(0).start()
    volt_copy(1).start()
    dft_copy.start()

    square = (chan_count, chan_count)
    row = lax.broadcasted_iota(jnp.int32, square, 0)
    column = lax.broadcasted_iota(jnp.int32, square, 1)
    mask = mask_ref[...].astype(jnp.float32)
    counted = jnp.where(column < row, mask, jnp.where(column == row, (1.0 - mask) * chan_count, 0.0))
    ones = jnp.ones((chan_count, 2 * LANES), jnp.bfloat16)
    order = jnp.dot(counted.astype(jnp.bfloat16), ones, preferred_element_type=jnp.float32)
    lane = lax.broadcasted_iota(jnp.int32, (chan_count, 2 * LANES), 1)
    slot_of = lax.rem(lane, SLOTS).astype(jnp.float32)
    picked = jnp.where(order == slot_of, 1.0, 0.0).astype(jnp.bfloat16)
    low_ref[...] = jnp.dot(
        jnp.broadcast_to(rate_ref[...].astype(jnp.float32), (8, chan_count)).astype(jnp.bfloat16),
        picked[:, :LANES],
        preferred_element_type=jnp.float32,
    )
    trig_copy.wait()
    cosines = jnp.dot(trig[0], picked, preferred_element_type=jnp.float32)
    sines = jnp.dot(trig[1], picked, preferred_element_type=jnp.float32)
    pl.semaphore_wait(barrier, tm_count + chan_devices)

    halo_copy = pltpu.make_async_remote_copy(
        src_ref=volt.at[:, :, pl.ds(0, HALO_ROWS), :],
        dst_ref=halo,
        send_sem=halo_sem.at[0],
        recv_sem=halo_sem.at[1],
        device_id=before_id,
        device_id_type=MESH,
    )

    @pl.when(place > 0)
    def _():
        halo_copy.start()

    imag = lax.rem(lane // 64, 2) == 1
    upper = jnp.where(imag, -sines, cosines)
    lower = jnp.where(imag, cosines, sines)
    taps = taps_ref[...] * chan_count ** (-0.5)
    taps_high = taps.astype(jnp.bfloat16)
    taps_low = (taps - taps_high.astype(jnp.float32)).astype(jnp.bfloat16)
    taps_pair = jnp.concatenate([taps_high.astype(jnp.float32), taps_low.astype(jnp.float32)], axis=0)
    taps_pair = taps_pair.T.astype(jnp.bfloat16)
    for pol in range(2):
        factor = jnp.dot(taps_pair, tap_ref[pol], preferred_element_type=jnp.float32)
        weight[pol, :chan_count] = (upper * factor).astype(jnp.bfloat16)
        weight[pol, chan_count:] = (lower * factor).astype(jnp.bfloat16)

    grams = ((g00, g01), (g10, g11))
    chunk = 256
    per_chunk = chunk // SHORT
    first_pol = lax.rem(lax.broadcasted_iota(jnp.int32, (per_chunk, LANES), 1) // SLOTS, 2) == 0
    sign_of = lambda n: jnp.where(
        lax.broadcasted_iota(jnp.int32, (n, LANES), 1) < LANES // 2, 1.0, -1.0
    ).astype(jnp.float32)

    def matmuls(slot, start):
        for pol in range(2):
            left, right = grams[pol]
            part = jnp.dot(
                jnp.concatenate(
                    [vbuf[slot, 2 * pol, start : start + chunk], vbuf[slot, 2 * pol + 1, start : start + chunk]],
                    axis=1,
                ),
                weight[pol],
                preferred_element_type=jnp.float32,
            )
            left[start : start + chunk] = part[:, :LANES]
            right[start : start + chunk] = part[:, LANES:]

    def combine(i, start):
        def both(at):
            low = pl.ds(start + at, per_chunk, stride=SHORT)
            high = pl.ds(start + at + 2, per_chunk, stride=SHORT)
            return g00[low, :] + g01[high, :], g10[low, :] + g11[high, :]

        here = both(0)
        where = pl.ds(pl.multiple_of(core * count + start // SHORT, per_chunk), per_chunk)
        for at in range(SHORT):
            later = both(at + 1)
            value = jnp.where(
                first_pol,
                here[0] + pltpu.roll(later[0], LANES - SLOTS, 1),
                here[1] + pltpu.roll(later[1], SLOTS, 1),
            )
            spec[i, at, where, :] = value.astype(jnp.bfloat16)
            here = later

    def swap(i):
        half = pl.ds(pl.multiple_of(core * count, count), count)
        return pltpu.make_async_remote_copy(
            src_ref=spec.at[i, :, half, :],
            dst_ref=spec.at[i + 1, :, half, :],
            send_sem=swap_sent.at[i // 2],
            recv_sem=swap_came.at[i // 2],
            device_id=(tm, chan + 1 - 2 * core),
            device_id_type=MESH,
        )

    def fine(i, item):
        sign_full = sign_of(LANES)
        for at in range(SHORT):
            plain = spec[i, at]
            flipped = (pltpu.roll(plain.astype(jnp.float32), LANES // 2, 1) * sign_full).astype(jnp.bfloat16)
            mid[at] = jnp.dot(
                dft[at], jnp.concatenate([plain, flipped], axis=0), preferred_element_type=jnp.float32
            )
        step = 16
        sign = sign_of(step)

        @pl.loop(0, LANES // step)
        def _(block):
            at_row = pl.multiple_of(block * step, step)
            spectra = short_dft([mid[at, pl.ds(at_row, step), :] for at in range(SHORT)], sign)
            for high, value in enumerate(spectra):
                where = pl.ds(pl.multiple_of(high // 2 * LANES + at_row, step), step)
                power[where, high % 2 * LANES : (high % 2 + 1) * LANES] = (value * value).astype(jnp.bfloat16)

        for pair in range(FINE // BLOCK // 2):
            sums = lax.dot_general(
                pick_ref[...],
                power[pair * BLOCK : (pair + 1) * BLOCK, :],
                (((1,), (1,)), ((), ())),
                preferred_element_type=jnp.float32,
            )
            for group in range(chan_devices):
                for side in range(2):
                    send[item, group, 2 * pair + side] = sums[
                        group * 8 : group * 8 + 8, side * LANES : (side + 1) * LANES
                    ].astype(jnp.bfloat16)

    def along_chan(item, k):
        return pltpu.make_async_remote_copy(
            src_ref=send.at[item, chan_peers[k]],
            dst_ref=held.at[item, k],
            send_sem=sent1.at[item, k],
            recv_sem=came1.at[item, k],
            device_id=(tm, chan_peers[k]),
            device_id_type=MESH,
        )

    def along_tm(item, k, q):
        block = held.at[item, k] if k else send.at[item, chan]
        return pltpu.make_async_remote_copy(
            src_ref=block.at[pl.ds(first_block(tm_peers[q]), 4)],
            dst_ref=out_ref.at[tm, chan_from[k], item],
            send_sem=sent2.at[item, k, q],
            recv_sem=came2.at[item, k, q],
            device_id=(tm_peers[q], chan),
            device_id_type=MESH,
        )

    def forward(item):
        for k in range(chan_devices):
            if k:
                along_chan(item, k).wait_recv()
            for q in range(1, tm_count):
                along_tm(item, k, q).start()
            near = pl.ds(first_block(tm), 4)
            out_ref[tm, chan_from[k], item] = held[item, k, near] if k else send[item, chan, near]

    @pl.loop(0, beams)
    def _(i):
        slot = lax.rem(i, DEPTH)
        item = i // 2
        beam = lax.rem(core + 1 + i, 2) * items + item
        volt_copy(i).wait()

        @pl.when(i + 2 < beams)
        def _():
            volt_copy(i + 2).start()

        for start in range(0, rows, chunk):
            matmuls(slot, start)
            if start:
                combine(i, start - chunk)

        @pl.when(i == 0)
        def _():
            @pl.when(place < last_place)
            def _():
                halo_copy.wait_recv()

            @pl.when(place == last_place)
            def _():
                halo[...] = jnp.zeros_like(halo)

            for pol in range(2):
                part = jnp.dot(
                    jnp.concatenate(
                        [
                            halo[:, 2 * pol].reshape(beams * HALO_ROWS, chan_count),
                            halo[:, 2 * pol + 1].reshape(beams * HALO_ROWS, chan_count),
                        ],
                        axis=1,
                    ),
                    weight[pol],
                    preferred_element_type=jnp.float32,
                )
                edge[pol] = part

        here = pl.ds(pl.multiple_of(beam * HALO_ROWS, HALO_ROWS), HALO_ROWS)
        for pol in range(2):
            left, right = grams[pol]
            left[rows : rows + HALO_ROWS] = edge[pol, here, :LANES]
            right[rows : rows + HALO_ROWS] = edge[pol, here, LANES:]
        combine(i, rows - chunk)

        @pl.when(lax.rem(i, 2) == 0)
        def _():
            swap(i).start()

        @pl.when(lax.rem(i, 2) == 1)
        def _():
            @pl.when(i == 1)
            def _():
                dft_copy.wait()

            swap(i - 1).wait_recv()
            fine(i, item)
            for k in range(1, chan_devices):
                along_chan(item, k).start()

            @pl.when(item > 0)
            def _():
                forward(item - 1)

    forward(items - 1)

    @pl.when(place > 0)
    def _():
        halo_copy.wait_send()

    @pl.loop(0, items)
    def _(item):
        swap(2 * item).wait_send()
        for k in range(chan_devices):
            if k:
                along_chan(item, k).wait_send()
            for q in range(1, tm_count):
                along_tm(item, k, q).wait_send()
        for k in range(chan_devices):
            for q in range(1, tm_count):
                pltpu.make_async_remote_copy(
                    src_ref=held.at[item, k, pl.ds(0, 4)],
                    dst_ref=out_ref.at[tm_from[q], chan_from[k], item],
                    send_sem=sent2.at[item, k, q],
                    recv_sem=came2.at[item, k, q],
                    device_id=(tm_peers[q], chan),
                    device_id_type=MESH,
                ).wait_recv()


def front(voltages, taps, busy_mask, drift_low, tm_count, chan_devices):
    beams, lanes, rows, chan_count = voltages.shape
    items = beams // 2
    ids = np.arange(chan_count)
    angles = (ids[:, None] * ids[None, :] % chan_count) * (2.0 * math.pi / chan_count)
    trig = jnp.asarray(np.stack([np.cos(angles), np.sin(angles)]), jnp.bfloat16)
    position = np.arange(SHORT)[:, None, None] + SHORT * np.arange(LANES)[None, None, :]
    turns = (position * np.arange(LANES)[None, :, None] % FINE) * (2.0 * math.pi / FINE)
    dft = jnp.asarray(np.concatenate([np.cos(turns), np.sin(turns)], axis=2), jnp.bfloat16)
    column = np.arange(2 * LANES)
    tap_of = np.stack([2 * (column // LANES) + (column // SLOTS % 2 ^ pol) for pol in range(2)])
    tap_pick = tap_of[:, None, :] == (np.arange(2 * TAPS) % TAPS)[None, :, None]
    per_group = SLOTS // chan_devices
    line = np.arange(8 * chan_devices)
    group, side, slot = line // 8, line % 8 // per_group, line % per_group
    lane = np.arange(2 * LANES)
    pick = (side[:, None] == lane[None, :] // LANES) & (
        (group * per_group + slot)[:, None] == lane[None, :] % SLOTS
    )
    vmem = pl.BlockSpec(memory_space=pltpu.VMEM)
    hbm = pl.BlockSpec(memory_space=pl.ANY)
    dma = pltpu.SemaphoreType.DMA
    kernel = lambda *refs: front_kernel(tm_count, chan_devices, *refs)
    blocks = FINE // BLOCK
    gram = pltpu.VMEM((rows + 3 * HALO_ROWS, LANES), jnp.float32)
    return pl.pallas_call(
        kernel,
        in_specs=[hbm, vmem, vmem, vmem, hbm, hbm, vmem, vmem],
        out_specs=(vmem, vmem),
        out_shape=(
            jax.ShapeDtypeStruct((tm_count, chan_devices, items, 4, 8, LANES), jnp.bfloat16),
            jax.ShapeDtypeStruct((8, LANES), jnp.float32),
        ),
        scratch_shapes=[
            pltpu.VMEM((DEPTH, lanes, rows, chan_count), jnp.bfloat16),
            pltpu.VMEM((beams, lanes, HALO_ROWS, chan_count), jnp.bfloat16),
            pltpu.VMEM(trig.shape, jnp.bfloat16),
            pltpu.VMEM(dft.shape, jnp.bfloat16),
            pltpu.VMEM((2, 2 * chan_count, 2 * LANES), jnp.bfloat16),
            pltpu.VMEM((2, beams * HALO_ROWS, 2 * LANES), jnp.float32),
            gram,
            gram,
            gram,
            gram,
            pltpu.VMEM((beams, SHORT, LANES, LANES), jnp.bfloat16),
            pltpu.VMEM((SHORT, LANES, LANES), jnp.float32),
            pltpu.VMEM((FINE // 2, 2 * LANES), jnp.bfloat16),
            pltpu.VMEM((items, chan_devices, blocks, 8, LANES), jnp.bfloat16),
            pltpu.VMEM((items, chan_devices, blocks, 8, LANES), jnp.bfloat16),
            dma((DEPTH,)),
            dma((2,)),
            dma((2,)),
            dma((items,)),
            dma((items,)),
            dma((items, chan_devices)),
            dma((items, chan_devices)),
            dma((items, chan_devices, tm_count)),
            dma((items, chan_devices, tm_count)),
        ],
        compiler_params=pltpu.CompilerParams(
            collective_id=0, has_side_effects=True, vmem_limit_bytes=56 * 2**20
        ),
    )(
        voltages,
        taps,
        busy_mask.reshape(1, chan_count),
        drift_low.reshape(1, chan_count),
        trig,
        dft,
        jnp.asarray(tap_pick, jnp.bfloat16),
        jnp.asarray(pick, jnp.bfloat16),
    )


STRIDE = 40


def drift_kernel(scale, place_ref, low_ref, in_ref, out_ref, rows_ref, stage_ref):
    steps, beams, tiles, _, _ = in_ref.shape
    _, _, rates, width = out_ref.shape
    slots = rows_ref.shape[0]
    pad = PAD // LANES
    wide = 2 * tiles
    out_tiles = width // LANES
    slot = pl.program_id(0)

    @pl.when(slot == 0)
    def _():
        empty = jnp.zeros((beams, LANES), jnp.float32)

        @pl.loop(0, steps)
        def _(t):
            for beam in range(beams):
                stage_ref[beam * STRIDE : beam * STRIDE + 8 * tiles] = (
                    in_ref[t, beam].astype(jnp.float32).reshape(8 * tiles, LANES)
                )
            for at in range(slots):
                for tile in range(pad):
                    rows_ref[at, t, tile] = empty
                    rows_ref[at, t, pad + wide + tile] = empty
                for tile in range(wide):
                    rows_ref[at, t, pad + tile] = stage_ref[pl.ds(tile * slots + at, beams, stride=STRIDE), :]

    lane8 = lax.broadcasted_iota(jnp.int32, (8, LANES), 1)
    low = jnp.sum(jnp.where(lane8 == place_ref[0] + slot, low_ref[...], 0.0)[:1]).astype(jnp.int32)
    lane = lax.broadcasted_iota(jnp.int32, (beams, LANES), 1)
    origin = place_ref[1] + PAD
    for rate in range(rates):
        totals = None
        for t in range(steps):
            start = (low * t + origin) + rate * t
            base = lax.shift_right_logical(start, 7)
            rest = start & (LANES - 1)
            parts = rows_ref[slot, t, pl.ds(base, out_tiles + (t > 0))]
            if t:
                keep = lane >= rest
                back = (LANES - rest) & (LANES - 1)
                parts = [
                    pltpu.roll(jnp.where(keep, parts[k], parts[k + 1]), back, 1) for k in range(out_tiles)
                ]
                totals = [total + part for total, part in zip(totals, parts)]
            else:
                totals = [parts[k] for k in range(out_tiles)]
        out_ref[:, 0, rate, :] = jnp.concatenate(totals, axis=1) * scale


def drift_sums(arrived, low_rates, place, slots, width):
    steps, beams, tiles, _, _ = arrived.shape
    kernel = lambda *refs: drift_kernel(1.0 / (4.0 * FINE * steps), *refs)
    vmem = pl.BlockSpec(memory_space=pltpu.VMEM)
    return pl.pallas_call(
        kernel,
        grid=(slots,),
        in_specs=[pl.BlockSpec(memory_space=pltpu.SMEM), vmem, vmem],
        out_specs=pl.BlockSpec((beams, 1, NDRIFT, width), lambda s: (0, s, 0, 0)),
        out_shape=jax.ShapeDtypeStruct((beams, slots, NDRIFT, width), jnp.float32),
        scratch_shapes=[
            pltpu.VMEM((slots, steps, 2 * tiles + 2 * PAD // LANES + 1, beams, LANES), jnp.float32),
            pltpu.VMEM((beams * STRIDE, LANES), jnp.float32),
        ],
        compiler_params=pltpu.CompilerParams(vmem_limit_bytes=48 * 2**20),
    )(place, low_rates, arrived)


def paired_shards(voltages, taps, busy_mask, drift_low):
    tm_count = lax.axis_size("tm")
    chan_devices = lax.axis_size("chan")
    beams = voltages.shape[0]
    slots = SLOTS // chan_devices
    arrived, low_rates = front(voltages, taps, busy_mask, drift_low, tm_count, chan_devices)
    arrived = arrived.reshape(tm_count * chan_devices // 2, beams, 4, 8, LANES)
    tm, chan = lax.axis_index("tm"), lax.axis_index("chan")
    width = FINE // tm_count
    place = jnp.stack([chan * slots, tm * width - BLOCK * first_block(tm)])
    return drift_sums(arrived, low_rates, place, slots, width)


def two_devices_hold_a_step(mesh, voltages):
    tm_count, chan_devices = mesh.shape["tm"], mesh.shape["chan"]
    rows = voltages.shape[2] // (tm_count * chan_devices)
    return (
        2 * rows == FINE
        and tm_count == 4
        and chan_devices == 2 * FSTEP
        and CH_DEV * tm_count * chan_devices == SLOTS
        and voltages.shape[0] == 8
        and PAD >= DSPAN * (FSTEP * tm_count - 1)
    )


def solution(mesh):
    in_specs = (P(None, None, ("tm", "chan"), None), P(), P(), P())
    out_specs = P(None, "chan", None, "tm")

    def run(voltages, taps, busy_mask, drift_low):
        body = paired_shards if two_devices_hold_a_step(mesh, voltages) else shards
        return jax.shard_map(
            body, mesh=mesh, in_specs=in_specs, out_specs=out_specs, check_vma=False
        )(voltages, taps, busy_mask, drift_low)

    return run
```

```python
import math

import jax
import jax.numpy as jnp
import numpy as np
from jax import lax
from jax.experimental import pallas as pl
from jax.experimental.pallas import tpu as pltpu
from jax.sharding import PartitionSpec as P

FA = 32
FB = 64
TAPS = 4
NDRIFT = 16
DSPAN = 16
FSTEP = 4
CH_DEV = 1


def passed_along(block, axis, distance):
    devices = range(lax.axis_size(axis))
    route = [(i - distance, i) for i in devices if i - distance in devices]
    return lax.ppermute(block, axis, route)


def busy_index(busy_mask, busy_count):
    before = jnp.cumsum(busy_mask) - busy_mask
    slot_ids = jnp.arange(busy_count, dtype=jnp.int32)
    is_slot = (busy_mask[:, None] == 1) & (before[:, None] == slot_ids[None, :])
    positions = jnp.arange(busy_mask.shape[0], dtype=jnp.int32)
    return jnp.sum(jnp.where(is_slot, positions[:, None], 0), axis=0)


def real_dft(sample_pos, freq_ids, length):
    phase_index = sample_pos[:, None] * freq_ids[None, :] % length
    angles = phase_index.astype(jnp.float32) * (2.0 * math.pi / length)
    cosines = jnp.cos(angles)
    sine_table = jnp.sin(angles)
    upper = jnp.stack([cosines, -sine_table], axis=1)
    lower = jnp.stack([sine_table, cosines], axis=1)
    return jnp.stack([upper, lower], axis=0).astype(jnp.bfloat16)


def to_bfloat(values):
    return lax.optimization_barrier(values.astype(jnp.bfloat16)).astype(jnp.float32)


def detect_power(spectra):
    items, lanes, chan_rows, samples = spectra.shape
    step_count = samples // (FA * FB)
    shaped = spectra.reshape(items, 2, 2, chan_rows, step_count, FA, FB)
    short_ids = jnp.arange(FA, dtype=jnp.int32)
    long_ids = jnp.arange(FB, dtype=jnp.int32)
    first_pass = jnp.einsum(
        "xopctab,paqf->xoqctfb",
        shaped,
        real_dft(short_ids, short_ids, FA),
        preferred_element_type=jnp.float32,
    )
    twist = short_ids[:, None] * long_ids[None, :] % (FA * FB)
    twist_angles = twist.astype(jnp.float32) * (2.0 * math.pi / (FA * FB))
    twist_cos = jnp.cos(twist_angles)
    twist_sin = jnp.sin(twist_angles)
    real_part = first_pass[:, :, 0]
    imag_part = first_pass[:, :, 1]
    turned = jnp.stack(
        [
            real_part * twist_cos + imag_part * twist_sin,
            imag_part * twist_cos - real_part * twist_sin,
        ],
        axis=2,
    ).astype(jnp.bfloat16)
    second_pass = jnp.einsum(
        "xoqctfb,qbsg->xosctgf",
        turned,
        real_dft(long_ids, long_ids, FB),
        preferred_element_type=jnp.float32,
    )
    powers = jnp.sum(second_pass * second_pass, axis=(1, 2)) / (4.0 * FA * FB)
    return powers.reshape(items, chan_rows, step_count, FA * FB)


def drift_rows(step_rows, first_step, drift_rates, first_bin, bin_width, pad_width):
    padded = jnp.pad(step_rows, ((0, 0), (0, 0), (0, 0), (pad_width, pad_width)))
    chan_rows = step_rows.shape[1]
    rate_count = drift_rates.shape[1]
    running = jnp.zeros((step_rows.shape[0], chan_rows, rate_count, bin_width), jnp.float32)
    for row_index in range(step_rows.shape[2]):
        step_time = first_step + row_index
        power_row = padded[:, 0, row_index]
        windows = []
        for rate_pos in range(rate_count):
            start = pad_width + first_bin + drift_rates[0, rate_pos] * step_time
            windows.append(lax.dynamic_slice_in_dim(power_row, start, bin_width, 1))
        per_slot = [jnp.stack(windows, axis=1)]
        running = running + jnp.stack(per_slot, axis=1)
    return running


def slot_rates(slot_part, drift_low):
    one_hot = slot_part[:, None] == jnp.arange(drift_low.shape[0], dtype=jnp.int32)[None, :]
    low_rates = jnp.sum(jnp.where(one_hot, drift_low[None, :], 0), axis=1)
    return low_rates[:, None] + jnp.arange(NDRIFT, dtype=jnp.int32)[None, :]


def shards(voltages, taps, busy_mask, drift_low):
    tm_count = lax.axis_size("tm")
    chan_devices = lax.axis_size("chan")
    count_of_beams, lanes, spec_dev, chan_count = voltages.shape
    busy_count = CH_DEV * tm_count * chan_devices
    step_count = FSTEP * tm_count
    pad_width = DSPAN * (step_count - 1)
    slot_index = busy_index(busy_mask, busy_count)
    slot_order = (
        slot_index.reshape(chan_devices, tm_count, CH_DEV).transpose(1, 0, 2).reshape(busy_count)
    )
    coarse_dft = real_dft(jnp.arange(chan_count, dtype=jnp.int32), slot_order, chan_count)
    following = passed_along(voltages[:, :, : TAPS - 1], ("tm", "chan"), -1)
    extended = jnp.concatenate([voltages, following], axis=2)
    filtered = taps[0] * extended[:, :, 0:spec_dev]
    for tap_index in range(1, TAPS):
        filtered = filtered + taps[tap_index] * extended[:, :, tap_index : tap_index + spec_dev]
    filtered = filtered.astype(jnp.bfloat16).reshape(count_of_beams, 2, 2, spec_dev, chan_count)
    coarse = jnp.einsum(
        "bopsn,pnqr->boqrs", filtered, coarse_dft, preferred_element_type=jnp.float32
    )
    coarse = (
        (coarse * chan_count ** (-0.5))
        .astype(jnp.bfloat16)
        .reshape(count_of_beams, 4, busy_count, spec_dev)
    )
    arrived = lax.all_to_all(
        lax.all_to_all(coarse, "tm", split_axis=2, concat_axis=3, tiled=True),
        "chan",
        split_axis=2,
        concat_axis=3,
        tiled=True,
    )
    ordered = arrived.reshape(count_of_beams, 4, CH_DEV, chan_devices, tm_count, spec_dev)
    ordered = ordered.transpose(0, 1, 2, 4, 3, 5).reshape(
        count_of_beams, 4, CH_DEV, tm_count * chan_devices * spec_dev
    )
    powers = detect_power(ordered)
    first_slot = lax.axis_index("chan") * (CH_DEV * tm_count) + lax.axis_index("tm") * CH_DEV
    drift_rates = slot_rates(lax.dynamic_slice_in_dim(slot_index, first_slot, CH_DEV), drift_low)
    drift_total = jnp.zeros((count_of_beams, CH_DEV, NDRIFT, FA * FB), jnp.float32)
    for group_index in range(tm_count):
        step_rows = powers[:, :, group_index * FSTEP : (group_index + 1) * FSTEP]
        drift_total = drift_total + to_bfloat(
            drift_rows(step_rows, group_index * FSTEP, drift_rates, 0, FA * FB, pad_width)
        )
    result = lax.all_to_all(
        (drift_total / step_count).astype(jnp.bfloat16),
        "tm",
        split_axis=3,
        concat_axis=1,
        tiled=True,
    ).astype(jnp.float32)
    return result


LANES = 128
FINE = FA * FB
SHORT = FINE // LANES
SLOTS = 32
HALO_ROWS = 8
PAD = 256
BLOCK = 256
DEPTH = 3
PITCH = 20


def short_dft(values, last=False):
    count = len(values)
    if count == 1:
        return values
    even = short_dft(values[0::2])
    odd = short_dft(values[1::2])
    low, high = [], []
    for k in range(count // 2):
        (same, turned), (term, flip) = even[k], odd[k]
        angle = 2.0 * math.pi * k / count
        if 4 * k == count:
            term, flip = flip, -term if not last else None
        elif k:
            cos, sin = math.cos(angle), math.sin(angle)
            term, flip = term * cos + flip * sin, flip * cos - term * sin if not last else None
        if last:
            low.append(same + term)
            high.append(same - term)
        else:
            low.append((same + term, turned + flip))
            high.append((same - term, turned - flip))
    return low + high


def first_block(part):
    return jnp.clip(2 * part - 1, 0, (FINE - 2 * PAD) // BLOCK - 2)


def flipped_bits(value, bits):
    moved, step = value, 1
    while step <= bits:
        if bits & step:
            moved = moved + step - 2 * step * lax.rem(value // step, 2)
        step *= 2
    return moved


def front_kernel(
    tm_count, chan_devices, volt, taps_hbm, mask_hbm, rate_hbm, trig_hbm, dft_hbm, tap_hbm, pick_hbm,
    out_ref, low_out, taps_ref, mask_ref, rate_ref, tap_ref, pick_ref, low_ref, vbuf, head, trig, dft, weight, edge, came_edge, g00, g01, g10, g11, spec, mid, power,
    send, held, volt_sem, const_sem, small_sem, edge_sem, swap_sent, swap_came, sent1, came1, sent2, came2, near_sem,
):
    beams, lanes, rows, chan_count = volt.shape
    items = beams // 2
    count = rows // SHORT
    tm, chan = lax.axis_index("tm"), lax.axis_index("chan")
    core = lax.rem(chan, 2)
    place = tm * chan_devices + chan
    last_place = tm_count * chan_devices - 1
    MESH = pl.DeviceIdType.MESH
    tm_peers = [flipped_bits(tm, q) for q in range(tm_count)]
    chan_peers = [flipped_bits(chan, k) for k in range(chan_devices)]
    far_first = range(chan_devices - 1, 0, -1)
    before = lax.rem(place + last_place, last_place + 1)
    after = lax.rem(place + 1, last_place + 1)
    before_id = (before // chan_devices, lax.rem(before, chan_devices))
    after_id = (after // chan_devices, lax.rem(after, chan_devices))

    barrier = pltpu.get_barrier_semaphore()
    for q in range(1, tm_count):
        pl.semaphore_signal(barrier, inc=1, device_id=(tm_peers[q], chan), device_id_type=MESH)
    for k in range(1, chan_devices):
        pl.semaphore_signal(barrier, inc=1, device_id=(tm, chan_peers[k]), device_id_type=MESH)
    pl.semaphore_signal(barrier, inc=1, device_id=before_id, device_id_type=MESH)
    pl.semaphore_signal(barrier, inc=1, device_id=after_id, device_id_type=MESH)

    def beam_of(i):
        return lax.rem(core + 1 + i, 2) * items + i // 2

    def volt_copy(i):
        slot = lax.rem(i, DEPTH)
        return pltpu.make_async_copy(volt.at[beam_of(i)], vbuf.at[slot], volt_sem.at[slot])

    trig_copy = pltpu.make_async_copy(trig_hbm, trig, const_sem.at[0])
    dft_copy = pltpu.make_async_copy(dft_hbm, dft, const_sem.at[1])
    head_copy = pltpu.make_async_copy(volt.at[:, :, pl.ds(0, HALO_ROWS), :], head, const_sem.at[2])
    smalls = [
        pltpu.make_async_copy(source, target, small_sem.at[n])
        for n, (source, target) in enumerate(
            ((mask_hbm, mask_ref), (rate_hbm, rate_ref), (taps_hbm, taps_ref), (tap_hbm, tap_ref), (pick_hbm, pick_ref))
        )
    ]
    for copy in smalls:
        copy.start()
    trig_copy.start()
    head_copy.start()
    volt_copy(0).start()
    for copy in smalls:
        copy.wait()

    square = (chan_count, chan_count)
    row = lax.broadcasted_iota(jnp.int32, square, 0)
    column = lax.broadcasted_iota(jnp.int32, square, 1)
    mask = mask_ref[...].astype(jnp.float32)
    counted = jnp.where(column < row, mask, jnp.where(column == row, (1.0 - mask) * chan_count, 0.0))
    ones = jnp.ones((chan_count, 2 * LANES), jnp.bfloat16)
    order = jnp.dot(counted.astype(jnp.bfloat16), ones, preferred_element_type=jnp.float32)
    lane = lax.broadcasted_iota(jnp.int32, (chan_count, 2 * LANES), 1)
    slot_of = lax.rem(lane, SLOTS).astype(jnp.float32)
    picked = jnp.where(order == slot_of, 1.0, 0.0).astype(jnp.bfloat16)
    low_ref[...] = jnp.dot(
        jnp.broadcast_to(rate_ref[...].astype(jnp.float32), (8, chan_count)).astype(jnp.bfloat16),
        picked[:, :LANES],
        preferred_element_type=jnp.float32,
    )
    low_copy = pltpu.make_async_copy(low_ref, low_out, small_sem.at[0])
    trig_copy.wait()
    cosines = jnp.dot(trig[0], picked, preferred_element_type=jnp.float32)
    sines = jnp.dot(trig[1], picked, preferred_element_type=jnp.float32)
    imag = lax.rem(lane // 64, 2) == 1
    upper = jnp.where(imag, -sines, cosines)
    lower = jnp.where(imag, cosines, sines)
    taps = taps_ref[...] * chan_count ** (-0.5)
    taps_high = taps.astype(jnp.bfloat16).astype(jnp.float32)
    taps_pair = jnp.concatenate([taps_high, taps - taps_high], axis=0).T.astype(jnp.bfloat16)
    for pol in range(2):
        factor = jnp.dot(taps_pair, tap_ref[pol], preferred_element_type=jnp.float32)
        weight[pol, :chan_count] = (upper * factor).astype(jnp.bfloat16)
        weight[pol, chan_count:] = (lower * factor).astype(jnp.bfloat16)
    volt_copy(1).start()
    dft_copy.start()
    low_copy.start()

    grams = ((g00, g01), (g10, g11))
    for left, right in grams:
        left[count * PITCH : count * PITCH + SHORT] = jnp.zeros((SHORT, LANES), jnp.float32)
        right[count * PITCH : count * PITCH + SHORT] = jnp.zeros((SHORT, LANES), jnp.float32)
    chunk = 256
    per_chunk = chunk // SHORT
    pol_of = lambda n: lax.rem(lax.broadcasted_iota(jnp.int32, (n, LANES), 1) // SLOTS, 2) == 0
    first_pol = pol_of(per_chunk)
    sign_of = lambda n: jnp.where(
        lax.broadcasted_iota(jnp.int32, (n, LANES), 1) < LANES // 2, 1.0, -1.0
    ).astype(jnp.float32)

    head_copy.wait()
    heads = beams * HALO_ROWS
    parts = []
    for pol in range(2):
        both_parts = [head[:, 2 * pol + p].reshape(heads, chan_count) for p in range(2)]
        parts.append(
            jnp.dot(jnp.concatenate(both_parts, axis=1), weight[pol], preferred_element_type=jnp.float32)
        )
    is_first = pol_of(heads)
    merged = lambda side: jnp.where(
        is_first, parts[0][:, side * LANES : (side + 1) * LANES], parts[1][:, side * LANES : (side + 1) * LANES]
    )
    moved = lambda side: jnp.where(
        is_first,
        pltpu.roll(parts[0][:, side * LANES : (side + 1) * LANES], LANES - SLOTS, 1),
        pltpu.roll(parts[1][:, side * LANES : (side + 1) * LANES], SLOTS, 1),
    )
    line = lax.rem(lax.broadcasted_iota(jnp.int32, (heads, LANES), 0), HALO_ROWS)
    edge[...] = (
        moved(1)
        + jnp.where(line >= 1, pltpu.roll(merged(1), 1, 0), 0.0)
        + jnp.where(line >= 2, pltpu.roll(moved(0), 2, 0), 0.0)
    )
    edge_copy = pltpu.make_async_remote_copy(
        src_ref=edge,
        dst_ref=came_edge,
        send_sem=edge_sem.at[0],
        recv_sem=edge_sem.at[1],
        device_id=before_id,
        device_id_type=MESH,
    )
    pl.semaphore_wait(barrier, tm_count + chan_devices)

    @pl.when(place > 0)
    def _():
        edge_copy.start()

    def matmuls(slot, start):
        for pol in range(2):
            left, right = grams[pol]
            part = jnp.dot(
                jnp.concatenate(
                    [vbuf[slot, 2 * pol, start : start + chunk], vbuf[slot, 2 * pol + 1, start : start + chunk]],
                    axis=1,
                ),
                weight[pol],
                preferred_element_type=jnp.float32,
            )
            for m in range(per_chunk):
                at = (start // SHORT + m) * PITCH
                left[at : at + SHORT] = part[m * SHORT : (m + 1) * SHORT, :LANES]
                right[at : at + SHORT] = part[m * SHORT : (m + 1) * SHORT, LANES:]

    def combine(i, start):
        def rows_at(at):
            return pl.ds((start // SHORT + at // SHORT) * PITCH + at % SHORT, per_chunk, stride=PITCH)

        def both(at):
            low, high = rows_at(at), rows_at(at + 2)
            return g00[low, :] + g01[high, :], g10[low, :] + g11[high, :]

        here = both(0)
        where = pl.ds(pl.multiple_of(core * count + start // SHORT, per_chunk), per_chunk)
        for at in range(SHORT):
            later = both(at + 1)
            value = jnp.where(
                first_pol,
                here[0] + pltpu.roll(later[0], LANES - SLOTS, 1),
                here[1] + pltpu.roll(later[1], SLOTS, 1),
            )
            spec[i, at, where, :] = value.astype(jnp.bfloat16)
            here = later

    def patch(i):
        where = pl.ds(pl.multiple_of(core * count + count - per_chunk, per_chunk), per_chunk)
        rows8 = came_edge[pl.ds(pl.multiple_of(beam_of(i) * HALO_ROWS, HALO_ROWS), HALO_ROWS), :]
        final = lax.broadcasted_iota(jnp.int32, (per_chunk, LANES), 0) == per_chunk - 1
        for n in range(TAPS - 1):
            at = SHORT - TAPS + 1 + n
            more = jnp.where(final, jnp.broadcast_to(rows8[n : n + 1], (per_chunk, LANES)), 0.0)
            spec[i, at, where, :] = (spec[i, at, where, :].astype(jnp.float32) + more).astype(jnp.bfloat16)

    def swap(i):
        half = pl.ds(pl.multiple_of(core * count, count), count)
        return pltpu.make_async_remote_copy(
            src_ref=spec.at[i, :, half, :],
            dst_ref=spec.at[i + 1, :, half, :],
            send_sem=swap_sent.at[i // 2],
            recv_sem=swap_came.at[i // 2],
            device_id=(tm, chan + 1 - 2 * core),
            device_id_type=MESH,
        )

    def fine_first(i):
        sign_full = sign_of(LANES).astype(jnp.bfloat16)
        for at in range(SHORT):
            plain = spec[i, at]
            flipped = pltpu.roll(plain, LANES // 2, 1) * sign_full
            mid[at, :LANES] = jnp.dot(
                dft[at],
                jnp.concatenate(
                    [jnp.concatenate([plain, flipped], axis=0), jnp.concatenate([flipped, -plain], axis=0)], axis=1
                ),
                preferred_element_type=jnp.float32,
            )

    def fine_second(at_row):
        rows8 = pl.ds(at_row, 8)
        spectra = short_dft([(mid[at, rows8, :LANES], mid[at, rows8, LANES:]) for at in range(SHORT)], True)
        for high, value in enumerate(spectra):
            where = pl.ds(high // 2 * LANES + at_row, 8)
            power[where, high % 2 * LANES : (high % 2 + 1) * LANES] = (value * value).astype(jnp.bfloat16)

    def fine_last(item):
        for pair in range(FINE // BLOCK // 2):
            sums = lax.dot_general(
                pick_ref[...],
                power[pair * BLOCK : (pair + 1) * BLOCK, :],
                (((1,), (1,)), ((), ())),
                preferred_element_type=jnp.float32,
            )
            for group in range(chan_devices):
                for side in range(2):
                    send[item, group, 2 * pair + side] = sums[
                        group * 8 : group * 8 + 8, side * LANES : (side + 1) * LANES
                    ].astype(jnp.bfloat16)

    def along_chan(item, k):
        return pltpu.make_async_remote_copy(
            src_ref=send.at[item, chan_peers[k]],
            dst_ref=held.at[item, k],
            send_sem=sent1.at[item, k],
            recv_sem=came1.at[item, k],
            device_id=(tm, chan_peers[k]),
            device_id_type=MESH,
        )

    def along_tm(item, k, q):
        block = held.at[item, k] if k else send.at[item, chan]
        return pltpu.make_async_remote_copy(
            src_ref=block.at[pl.ds(first_block(tm_peers[q]), 4)],
            dst_ref=out_ref.at[tm, chan_peers[k], item],
            send_sem=sent2.at[item, k, q],
            recv_sem=came2.at[item, k, q],
            device_id=(tm_peers[q], chan),
            device_id_type=MESH,
        )

    def near_copy(item, k):
        block = held.at[item, k] if k else send.at[item, chan]
        return pltpu.make_async_copy(
            block.at[pl.ds(first_block(tm), 4)], out_ref.at[tm, chan_peers[k], item], near_sem.at[item, k]
        )

    def forward(item):
        for k in range(chan_devices):
            if k:
                along_chan(item, k).wait_recv()
            for q in range(tm_count - 1, 0, -1):
                along_tm(item, k, q).start()
            near_copy(item, k).start()

    def coarse_start(i):
        volt_copy(i).wait()

        @pl.when(i + 2 < beams)
        def _():
            volt_copy(i + 2).start()

    def coarse_rest(i):
        for start in range(chunk, rows, chunk):
            matmuls(lax.rem(i, DEPTH), start)
            combine(i, start - chunk)

    def share(item):
        for k in far_first:
            along_chan(item, k).start()

        @pl.when(item > 0)
        def _():
            forward(item - 1)

    @pl.loop(0, items)
    def _(pair):
        i = 2 * pair
        done = jnp.maximum(i - 1, 0)
        item = jnp.maximum(pair - 1, 0)
        coarse_start(i)
        matmuls(lax.rem(i, DEPTH), 0)
        combine(done, rows - chunk)

        @pl.when(pair == 0)
        def _():
            coarse_rest(i)

        @pl.when(pair > 0)
        def _():
            @pl.when(pair == 1)
            def _():
                dft_copy.wait()

            patch(i - 1)
            swap(i - 2).wait_recv()
            fine_first(done)
            groups = list(range(0, LANES, 8))
            for start in range(chunk, rows, chunk):
                matmuls(lax.rem(i, DEPTH), start)
                combine(i, start - chunk)
                share_of = len(groups) // ((rows - start) // chunk)
                for at_row in groups[:share_of]:
                    fine_second(at_row)
                groups = groups[share_of:]
            fine_last(item)
            share(item)

        coarse_start(i + 1)
        matmuls(lax.rem(i + 1, DEPTH), 0)
        combine(i, rows - chunk)

        @pl.when(pair == 0)
        def _():
            @pl.when(place < last_place)
            def _():
                edge_copy.wait_recv()

            @pl.when(place == last_place)
            def _():
                came_edge[...] = jnp.zeros_like(came_edge)

        patch(i)
        swap(i).start()
        coarse_rest(i + 1)

    combine(beams - 1, rows - chunk)
    patch(beams - 1)
    swap(beams - 2).wait_recv()
    fine_first(beams - 1)

    for at_row in range(0, LANES, 8):
        fine_second(at_row)
    fine_last(items - 1)
    share(items - 1)
    forward(items - 1)

    low_copy.wait()

    @pl.when(place > 0)
    def _():
        edge_copy.wait_send()

    @pl.loop(0, items)
    def _(item):
        swap(2 * item).wait_send()
        for k in range(chan_devices):
            if k:
                along_chan(item, k).wait_send()
            for q in range(1, tm_count):
                along_tm(item, k, q).wait_send()
            near_copy(item, k).wait()
        for k in range(chan_devices):
            for q in range(1, tm_count):
                pltpu.make_async_remote_copy(
                    src_ref=held.at[item, k, pl.ds(0, 4)],
                    dst_ref=out_ref.at[tm_peers[q], chan_peers[k], item],
                    send_sem=sent2.at[item, k, q],
                    recv_sem=came2.at[item, k, q],
                    device_id=(tm_peers[q], chan),
                    device_id_type=MESH,
                ).wait_recv()


def front(voltages, taps, busy_mask, drift_low, tm_count, chan_devices):
    beams, lanes, rows, chan_count = voltages.shape
    items = beams // 2
    ids = np.arange(chan_count)
    angles = (ids[:, None] * ids[None, :] % chan_count) * (2.0 * math.pi / chan_count)
    trig = jnp.asarray(np.stack([np.cos(angles), np.sin(angles)]), jnp.bfloat16)
    position = np.arange(SHORT)[:, None, None] + SHORT * np.arange(LANES)[None, None, :]
    turns = (position * np.arange(LANES)[None, :, None] % FINE) * (2.0 * math.pi / FINE)
    dft = jnp.asarray(np.concatenate([np.cos(turns), np.sin(turns)], axis=2), jnp.bfloat16)
    column = np.arange(2 * LANES)
    tap_of = np.stack([2 * (column // LANES) + (column // SLOTS % 2 ^ pol) for pol in range(2)])
    tap_pick = tap_of[:, None, :] == (np.arange(2 * TAPS) % TAPS)[None, :, None]
    per_group = SLOTS // chan_devices
    line = np.arange(8 * chan_devices)
    group, side, slot = line // 8, line % 8 // per_group, line % per_group
    lane = np.arange(2 * LANES)
    pick = (side[:, None] == lane[None, :] // LANES) & (
        (group * per_group + slot)[:, None] == lane[None, :] % SLOTS
    )
    hbm = pl.BlockSpec(memory_space=pl.ANY)
    dma = pltpu.SemaphoreType.DMA
    kernel = lambda *refs: front_kernel(tm_count, chan_devices, *refs)
    blocks = FINE // BLOCK
    gram = pltpu.VMEM(((rows // SHORT + 1) * PITCH, LANES), jnp.float32)
    return pl.pallas_call(
        kernel,
        in_specs=[hbm] * 8,
        out_specs=(hbm, hbm),
        out_shape=(
            jax.ShapeDtypeStruct((tm_count, chan_devices, items, 4, 8, LANES), jnp.bfloat16),
            jax.ShapeDtypeStruct((8, LANES), jnp.float32),
        ),
        scratch_shapes=[
            pltpu.VMEM(taps.shape, jnp.float32),
            pltpu.VMEM((1, chan_count), jnp.int32),
            pltpu.VMEM((1, chan_count), jnp.int32),
            pltpu.VMEM(tap_pick.shape, jnp.bfloat16),
            pltpu.VMEM(pick.shape, jnp.bfloat16),
            pltpu.VMEM((8, LANES), jnp.float32),
            pltpu.VMEM((DEPTH, lanes, rows, chan_count), jnp.bfloat16),
            pltpu.VMEM((beams, lanes, HALO_ROWS, chan_count), jnp.bfloat16),
            pltpu.VMEM(trig.shape, jnp.bfloat16),
            pltpu.VMEM(dft.shape, jnp.bfloat16),
            pltpu.VMEM((2, 2 * chan_count, 2 * LANES), jnp.bfloat16),
            pltpu.VMEM((beams * HALO_ROWS, LANES), jnp.float32),
            pltpu.VMEM((beams * HALO_ROWS, LANES), jnp.float32),
            gram,
            gram,
            gram,
            gram,
            pltpu.VMEM((beams, SHORT, LANES, LANES), jnp.bfloat16),
            pltpu.VMEM((SHORT, LANES + 8, 2 * LANES), jnp.float32),
            pltpu.VMEM((FINE // 2, 2 * LANES), jnp.bfloat16),
            pltpu.VMEM((items, chan_devices, blocks, 8, LANES), jnp.bfloat16),
            pltpu.VMEM((items, chan_devices, blocks, 8, LANES), jnp.bfloat16),
            dma((DEPTH,)),
            dma((3,)),
            dma((5,)),
            dma((2,)),
            dma((items,)),
            dma((items,)),
            dma((items, chan_devices)),
            dma((items, chan_devices)),
            dma((items, chan_devices, tm_count)),
            dma((items, chan_devices, tm_count)),
            dma((items, chan_devices)),
        ],
        compiler_params=pltpu.CompilerParams(
            collective_id=0, has_side_effects=True, vmem_limit_bytes=56 * 2**20
        ),
    )(
        voltages,
        taps,
        busy_mask.reshape(1, chan_count),
        drift_low.reshape(1, chan_count),
        trig,
        dft,
        jnp.asarray(tap_pick, jnp.bfloat16),
        jnp.asarray(pick, jnp.bfloat16),
    )


STRIDE = 40


def drift_kernel(scale, low_hbm, in_hbm, out_ref, low_ref, in_ref, rows_ref, stage_ref, sems):
    steps, beams, tiles, _, _ = in_ref.shape
    _, _, rates, width = out_ref.shape
    slots = rows_ref.shape[0]
    pad = PAD // LANES
    wide = 2 * tiles
    slot = pl.program_id(0)
    tm, chan = lax.axis_index("tm"), lax.axis_index("chan")
    parts = 4
    portion = steps // parts

    def arrival(n):
        span = pl.ds(n * portion, portion)
        return pltpu.make_async_copy(in_hbm.at[span], in_ref.at[span], sems.at[n])

    @pl.when(slot == 0)
    def _():
        low_copy = pltpu.make_async_copy(low_hbm, low_ref, sems.at[parts])
        for n in range(parts):
            arrival(n).start()
        low_copy.start()
        empty = jnp.zeros((beams, LANES), jnp.float32)

        @pl.loop(0, parts)
        def _(n):
            arrival(n).wait()

            @pl.loop(0, portion)
            def _(step):
                t = n * portion + step
                for beam in range(beams):
                    stage_ref[beam * STRIDE : beam * STRIDE + 8 * tiles] = (
                        in_ref[t, beam].astype(jnp.float32).reshape(8 * tiles, LANES)
                    )
                for at in range(slots):
                    rows = [empty] * pad
                    rows += [stage_ref[pl.ds(tile * slots + at, beams, stride=STRIDE), :] for tile in range(wide)]
                    rows += [empty] * pad
                    for tile in range(wide + 2 * pad - 2):
                        rows_ref[at, t, tile] = jnp.concatenate([rows[tile], rows[tile + 2]], axis=0).astype(
                            jnp.bfloat16
                        )

        low_copy.wait()

    lane8 = lax.broadcasted_iota(jnp.int32, (8, LANES), 1)
    low = jnp.sum(jnp.where(lane8 == chan * slots + slot, low_ref[...], 0.0)[:1]).astype(jnp.int32)
    lane = lax.broadcasted_iota(jnp.int32, (2 * beams, LANES), 1)
    origin = tm * width - BLOCK * first_block(tm) + PAD
    for rate in range(rates):
        totals = None
        for t in range(steps):
            start = (low * t + origin) + rate * t
            base = lax.shift_right_logical(start, 7)
            if t:
                rest = start & (LANES - 1)
                back = (LANES - rest) & (LANES - 1)
                keep = lane >= rest
                three = rows_ref[slot, t, pl.ds(base, 3)]
                even, odd = [
                    pltpu.roll(jnp.where(keep, three[k], three[k + 1]), back, 1).astype(jnp.float32) for k in range(2)
                ]
            else:
                two = rows_ref[slot, t, pl.ds(base, 2)]
                even, odd = two[0].astype(jnp.float32), two[1].astype(jnp.float32)
            added = [even[:beams], odd[:beams], even[beams:], odd[beams:]]
            totals = added if totals is None else [total + more for total, more in zip(totals, added)]
        out_ref[:, 0, rate, :] = jnp.concatenate(totals, axis=1) * scale


def drift_sums(arrived, low_rates, slots, width):
    steps, beams, tiles, _, _ = arrived.shape
    kernel = lambda *refs: drift_kernel(1.0 / (4.0 * FINE * steps), *refs)
    hbm = pl.BlockSpec(memory_space=pl.ANY)
    return pl.pallas_call(
        kernel,
        grid=(slots,),
        in_specs=[hbm, hbm],
        out_specs=pl.BlockSpec((beams, 1, NDRIFT, width), lambda s: (0, s, 0, 0)),
        out_shape=jax.ShapeDtypeStruct((beams, slots, NDRIFT, width), jnp.float32),
        scratch_shapes=[
            pltpu.VMEM((8, LANES), jnp.float32),
            pltpu.VMEM(arrived.shape, jnp.bfloat16),
            pltpu.VMEM((slots, steps, 2 * tiles + 2 * PAD // LANES - 2, 2 * beams, LANES), jnp.bfloat16),
            pltpu.VMEM((beams * STRIDE, LANES), jnp.float32),
            pltpu.SemaphoreType.DMA((5,)),
        ],
        compiler_params=pltpu.CompilerParams(vmem_limit_bytes=60 * 2**20),
    )(low_rates, arrived)


def paired_shards(voltages, taps, busy_mask, drift_low):
    tm_count = lax.axis_size("tm")
    chan_devices = lax.axis_size("chan")
    arrived, low_rates = front(voltages, taps, busy_mask, drift_low, tm_count, chan_devices)
    arrived = arrived.reshape(tm_count * chan_devices // 2, voltages.shape[0], 4, 8, LANES)
    return drift_sums(arrived, low_rates, SLOTS // chan_devices, FINE // tm_count)


def two_devices_hold_a_step(mesh, voltages):
    tm_count, chan_devices = mesh.shape["tm"], mesh.shape["chan"]
    rows = voltages.shape[2] // (tm_count * chan_devices)
    return (
        2 * rows == FINE
        and tm_count == 4
        and chan_devices == 2 * FSTEP
        and CH_DEV * tm_count * chan_devices == SLOTS
        and voltages.shape[0] == 8
        and PAD >= DSPAN * (FSTEP * tm_count - 1)
    )


def solution(mesh):
    in_specs = (P(None, None, ("tm", "chan"), None), P(), P(), P())
    out_specs = P(None, "chan", None, "tm")

    def run(voltages, taps, busy_mask, drift_low):
        body = paired_shards if two_devices_hold_a_step(mesh, voltages) else shards
        return jax.shard_map(
            body, mesh=mesh, in_specs=in_specs, out_specs=out_specs, check_vma=False
        )(voltages, taps, busy_mask, drift_low)

    return run
```

```python
import math

import jax
import jax.numpy as jnp
import numpy as np
from jax import lax
from jax.experimental import pallas as pl
from jax.experimental.pallas import tpu as pltpu
from jax.sharding import PartitionSpec as P

FA = 32
FB = 64
TAPS = 4
NDRIFT = 16
DSPAN = 16
FSTEP = 4
CH_DEV = 1


def passed_along(block, axis, distance):
    devices = range(lax.axis_size(axis))
    route = [(i - distance, i) for i in devices if i - distance in devices]
    return lax.ppermute(block, axis, route)


def busy_index(busy_mask, busy_count):
    before = jnp.cumsum(busy_mask) - busy_mask
    slot_ids = jnp.arange(busy_count, dtype=jnp.int32)
    is_slot = (busy_mask[:, None] == 1) & (before[:, None] == slot_ids[None, :])
    positions = jnp.arange(busy_mask.shape[0], dtype=jnp.int32)
    return jnp.sum(jnp.where(is_slot, positions[:, None], 0), axis=0)


def real_dft(sample_pos, freq_ids, length):
    phase_index = sample_pos[:, None] * freq_ids[None, :] % length
    angles = phase_index.astype(jnp.float32) * (2.0 * math.pi / length)
    cosines = jnp.cos(angles)
    sine_table = jnp.sin(angles)
    upper = jnp.stack([cosines, -sine_table], axis=1)
    lower = jnp.stack([sine_table, cosines], axis=1)
    return jnp.stack([upper, lower], axis=0).astype(jnp.bfloat16)


def to_bfloat(values):
    return lax.optimization_barrier(values.astype(jnp.bfloat16)).astype(jnp.float32)


def detect_power(spectra):
    items, lanes, chan_rows, samples = spectra.shape
    step_count = samples // (FA * FB)
    shaped = spectra.reshape(items, 2, 2, chan_rows, step_count, FA, FB)
    short_ids = jnp.arange(FA, dtype=jnp.int32)
    long_ids = jnp.arange(FB, dtype=jnp.int32)
    first_pass = jnp.einsum(
        "xopctab,paqf->xoqctfb",
        shaped,
        real_dft(short_ids, short_ids, FA),
        preferred_element_type=jnp.float32,
    )
    twist = short_ids[:, None] * long_ids[None, :] % (FA * FB)
    twist_angles = twist.astype(jnp.float32) * (2.0 * math.pi / (FA * FB))
    twist_cos = jnp.cos(twist_angles)
    twist_sin = jnp.sin(twist_angles)
    real_part = first_pass[:, :, 0]
    imag_part = first_pass[:, :, 1]
    turned = jnp.stack(
        [
            real_part * twist_cos + imag_part * twist_sin,
            imag_part * twist_cos - real_part * twist_sin,
        ],
        axis=2,
    ).astype(jnp.bfloat16)
    second_pass = jnp.einsum(
        "xoqctfb,qbsg->xosctgf",
        turned,
        real_dft(long_ids, long_ids, FB),
        preferred_element_type=jnp.float32,
    )
    powers = jnp.sum(second_pass * second_pass, axis=(1, 2)) / (4.0 * FA * FB)
    return powers.reshape(items, chan_rows, step_count, FA * FB)


def drift_rows(step_rows, first_step, drift_rates, first_bin, bin_width, pad_width):
    padded = jnp.pad(step_rows, ((0, 0), (0, 0), (0, 0), (pad_width, pad_width)))
    chan_rows = step_rows.shape[1]
    rate_count = drift_rates.shape[1]
    running = jnp.zeros((step_rows.shape[0], chan_rows, rate_count, bin_width), jnp.float32)
    for row_index in range(step_rows.shape[2]):
        step_time = first_step + row_index
        power_row = padded[:, 0, row_index]
        windows = []
        for rate_pos in range(rate_count):
            start = pad_width + first_bin + drift_rates[0, rate_pos] * step_time
            windows.append(lax.dynamic_slice_in_dim(power_row, start, bin_width, 1))
        per_slot = [jnp.stack(windows, axis=1)]
        running = running + jnp.stack(per_slot, axis=1)
    return running


def slot_rates(slot_part, drift_low):
    one_hot = slot_part[:, None] == jnp.arange(drift_low.shape[0], dtype=jnp.int32)[None, :]
    low_rates = jnp.sum(jnp.where(one_hot, drift_low[None, :], 0), axis=1)
    return low_rates[:, None] + jnp.arange(NDRIFT, dtype=jnp.int32)[None, :]


def shards(voltages, taps, busy_mask, drift_low):
    tm_count = lax.axis_size("tm")
    chan_devices = lax.axis_size("chan")
    count_of_beams, lanes, spec_dev, chan_count = voltages.shape
    busy_count = CH_DEV * tm_count * chan_devices
    step_count = FSTEP * tm_count
    pad_width = DSPAN * (step_count - 1)
    slot_index = busy_index(busy_mask, busy_count)
    slot_order = (
        slot_index.reshape(chan_devices, tm_count, CH_DEV).transpose(1, 0, 2).reshape(busy_count)
    )
    coarse_dft = real_dft(jnp.arange(chan_count, dtype=jnp.int32), slot_order, chan_count)
    following = passed_along(voltages[:, :, : TAPS - 1], ("tm", "chan"), -1)
    extended = jnp.concatenate([voltages, following], axis=2)
    filtered = taps[0] * extended[:, :, 0:spec_dev]
    for tap_index in range(1, TAPS):
        filtered = filtered + taps[tap_index] * extended[:, :, tap_index : tap_index + spec_dev]
    filtered = filtered.astype(jnp.bfloat16).reshape(count_of_beams, 2, 2, spec_dev, chan_count)
    coarse = jnp.einsum(
        "bopsn,pnqr->boqrs", filtered, coarse_dft, preferred_element_type=jnp.float32
    )
    coarse = (
        (coarse * chan_count ** (-0.5))
        .astype(jnp.bfloat16)
        .reshape(count_of_beams, 4, busy_count, spec_dev)
    )
    arrived = lax.all_to_all(
        lax.all_to_all(coarse, "tm", split_axis=2, concat_axis=3, tiled=True),
        "chan",
        split_axis=2,
        concat_axis=3,
        tiled=True,
    )
    ordered = arrived.reshape(count_of_beams, 4, CH_DEV, chan_devices, tm_count, spec_dev)
    ordered = ordered.transpose(0, 1, 2, 4, 3, 5).reshape(
        count_of_beams, 4, CH_DEV, tm_count * chan_devices * spec_dev
    )
    powers = detect_power(ordered)
    first_slot = lax.axis_index("chan") * (CH_DEV * tm_count) + lax.axis_index("tm") * CH_DEV
    drift_rates = slot_rates(lax.dynamic_slice_in_dim(slot_index, first_slot, CH_DEV), drift_low)
    drift_total = jnp.zeros((count_of_beams, CH_DEV, NDRIFT, FA * FB), jnp.float32)
    for group_index in range(tm_count):
        step_rows = powers[:, :, group_index * FSTEP : (group_index + 1) * FSTEP]
        drift_total = drift_total + to_bfloat(
            drift_rows(step_rows, group_index * FSTEP, drift_rates, 0, FA * FB, pad_width)
        )
    result = lax.all_to_all(
        (drift_total / step_count).astype(jnp.bfloat16),
        "tm",
        split_axis=3,
        concat_axis=1,
        tiled=True,
    ).astype(jnp.float32)
    return result


LANES = 128
FINE = FA * FB
SHORT = FINE // LANES
SLOTS = 32
HALO_ROWS = 8
PAD = 256
BLOCK = 256
DEPTH = 3
PITCH = 20


def short_dft(values, last=False):
    count = len(values)
    if count == 1:
        return values
    even = short_dft(values[0::2])
    odd = short_dft(values[1::2])
    low, high = [], []
    for k in range(count // 2):
        (same, turned), (term, flip) = even[k], odd[k]
        angle = 2.0 * math.pi * k / count
        if 4 * k == count:
            term, flip = flip, -term if not last else None
        elif k:
            cos, sin = math.cos(angle), math.sin(angle)
            term, flip = term * cos + flip * sin, flip * cos - term * sin if not last else None
        if last:
            low.append(same + term)
            high.append(same - term)
        else:
            low.append((same + term, turned + flip))
            high.append((same - term, turned - flip))
    return low + high


def first_block(part):
    return jnp.clip(2 * part - 1, 0, (FINE - 2 * PAD) // BLOCK - 2)


def flipped_bits(value, bits):
    moved, step = value, 1
    while step <= bits:
        if bits & step:
            moved = moved + step - 2 * step * lax.rem(value // step, 2)
        step *= 2
    return moved


def front_kernel(
    tm_count, chan_devices, volt, taps_hbm, mask_hbm, rate_hbm, trig_hbm, dft_hbm, tap_hbm, pick_hbm,
    out_ref, low_out, taps_ref, mask_ref, rate_ref, tap_ref, pick_ref, low_ref, vbuf, head, trig, dft, weight, edge, came_edge, g00, g01, g10, g11, spec, mid, power,
    send, held, volt_sem, const_sem, small_sem, edge_sem, swap_sent, swap_came, sent1, came1, sent2, came2, near_sem,
):
    beams, lanes, rows, chan_count = volt.shape
    items = beams // 2
    count = rows // SHORT
    tm, chan = lax.axis_index("tm"), lax.axis_index("chan")
    core = lax.rem(chan, 2)
    place = tm * chan_devices + chan
    last_place = tm_count * chan_devices - 1
    MESH = pl.DeviceIdType.MESH
    tm_peers = [flipped_bits(tm, q) for q in range(tm_count)]
    chan_peers = [flipped_bits(chan, k) for k in range(chan_devices)]
    far_first = range(chan_devices - 1, 0, -1)
    before = lax.rem(place + last_place, last_place + 1)
    after = lax.rem(place + 1, last_place + 1)
    before_id = (before // chan_devices, lax.rem(before, chan_devices))
    after_id = (after // chan_devices, lax.rem(after, chan_devices))

    barrier = pltpu.get_barrier_semaphore()
    for q in range(1, tm_count):
        pl.semaphore_signal(barrier, inc=1, device_id=(tm_peers[q], chan), device_id_type=MESH)
    for k in range(1, chan_devices):
        pl.semaphore_signal(barrier, inc=1, device_id=(tm, chan_peers[k]), device_id_type=MESH)
    pl.semaphore_signal(barrier, inc=1, device_id=before_id, device_id_type=MESH)
    pl.semaphore_signal(barrier, inc=1, device_id=after_id, device_id_type=MESH)

    def beam_of(i):
        return lax.rem(core + 1 + i, 2) * items + i // 2

    def volt_copy(i):
        slot = lax.rem(i, DEPTH)
        return pltpu.make_async_copy(volt.at[beam_of(i)], vbuf.at[slot], volt_sem.at[slot])

    trig_copy = pltpu.make_async_copy(trig_hbm, trig, const_sem.at[0])
    dft_copy = pltpu.make_async_copy(dft_hbm, dft, const_sem.at[1])
    head_copy = pltpu.make_async_copy(volt.at[:, :, pl.ds(0, HALO_ROWS), :], head, const_sem.at[2])
    smalls = [
        pltpu.make_async_copy(source, target, small_sem.at[n])
        for n, (source, target) in enumerate(
            ((mask_hbm, mask_ref), (rate_hbm, rate_ref), (taps_hbm, taps_ref), (tap_hbm, tap_ref), (pick_hbm, pick_ref))
        )
    ]
    for copy in smalls:
        copy.start()
    trig_copy.start()
    head_copy.start()
    volt_copy(0).start()
    for copy in smalls:
        copy.wait()

    square = (chan_count, chan_count)
    row = lax.broadcasted_iota(jnp.int32, square, 0)
    column = lax.broadcasted_iota(jnp.int32, square, 1)
    mask = mask_ref[...].astype(jnp.float32)
    counted = jnp.where(column < row, mask, jnp.where(column == row, (1.0 - mask) * chan_count, 0.0))
    ones = jnp.ones((chan_count, 2 * LANES), jnp.bfloat16)
    order = jnp.dot(counted.astype(jnp.bfloat16), ones, preferred_element_type=jnp.float32)
    lane = lax.broadcasted_iota(jnp.int32, (chan_count, 2 * LANES), 1)
    slot_of = lax.rem(lane, SLOTS).astype(jnp.float32)
    picked = jnp.where(order == slot_of, 1.0, 0.0).astype(jnp.bfloat16)
    low_ref[...] = jnp.dot(
        jnp.broadcast_to(rate_ref[...].astype(jnp.float32), (8, chan_count)).astype(jnp.bfloat16),
        picked[:, :LANES],
        preferred_element_type=jnp.float32,
    )
    low_copy = pltpu.make_async_copy(low_ref, low_out, small_sem.at[0])
    trig_copy.wait()
    cosines = jnp.dot(trig[0], picked, preferred_element_type=jnp.float32)
    sines = jnp.dot(trig[1], picked, preferred_element_type=jnp.float32)
    imag = lax.rem(lane // 64, 2) == 1
    upper = jnp.where(imag, -sines, cosines)
    lower = jnp.where(imag, cosines, sines)
    taps = taps_ref[...] * chan_count ** (-0.5)
    taps_high = taps.astype(jnp.bfloat16).astype(jnp.float32)
    taps_pair = jnp.concatenate([taps_high, taps - taps_high], axis=0).T.astype(jnp.bfloat16)
    for pol in range(2):
        factor = jnp.dot(taps_pair, tap_ref[pol], preferred_element_type=jnp.float32)
        weight[pol, :chan_count] = (upper * factor).astype(jnp.bfloat16)
        weight[pol, chan_count:] = (lower * factor).astype(jnp.bfloat16)
    volt_copy(1).start()
    dft_copy.start()
    low_copy.start()

    grams = ((g00, g01), (g10, g11))
    for left, right in grams:
        left[count * PITCH : count * PITCH + SHORT] = jnp.zeros((SHORT, LANES), jnp.float32)
        right[count * PITCH : count * PITCH + SHORT] = jnp.zeros((SHORT, LANES), jnp.float32)
    chunk = 256
    per_chunk = chunk // SHORT
    pol_of = lambda n: lax.rem(lax.broadcasted_iota(jnp.int32, (n, LANES), 1) // SLOTS, 2) == 0
    first_pol = pol_of(per_chunk)
    sign_of = lambda n: jnp.where(
        lax.broadcasted_iota(jnp.int32, (n, LANES), 1) < LANES // 2, 1.0, -1.0
    ).astype(jnp.float32)

    head_copy.wait()
    heads = beams * HALO_ROWS
    parts = []
    for pol in range(2):
        both_parts = [head[:, 2 * pol + p].reshape(heads, chan_count) for p in range(2)]
        parts.append(
            jnp.dot(jnp.concatenate(both_parts, axis=1), weight[pol], preferred_element_type=jnp.float32)
        )
    is_first = pol_of(heads)
    merged = lambda side: jnp.where(
        is_first, parts[0][:, side * LANES : (side + 1) * LANES], parts[1][:, side * LANES : (side + 1) * LANES]
    )
    moved = lambda side: jnp.where(
        is_first,
        pltpu.roll(parts[0][:, side * LANES : (side + 1) * LANES], LANES - SLOTS, 1),
        pltpu.roll(parts[1][:, side * LANES : (side + 1) * LANES], SLOTS, 1),
    )
    line = lax.rem(lax.broadcasted_iota(jnp.int32, (heads, LANES), 0), HALO_ROWS)
    edge[...] = (
        moved(1)
        + jnp.where(line >= 1, pltpu.roll(merged(1), 1, 0), 0.0)
        + jnp.where(line >= 2, pltpu.roll(moved(0), 2, 0), 0.0)
    )
    edge_copy = pltpu.make_async_remote_copy(
        src_ref=edge,
        dst_ref=came_edge,
        send_sem=edge_sem.at[0],
        recv_sem=edge_sem.at[1],
        device_id=before_id,
        device_id_type=MESH,
    )
    pl.semaphore_wait(barrier, tm_count + chan_devices)

    @pl.when(place > 0)
    def _():
        edge_copy.start()

    def matmuls(slot, start):
        for pol in range(2):
            left, right = grams[pol]
            part = jnp.dot(
                jnp.concatenate(
                    [vbuf[slot, 2 * pol, start : start + chunk], vbuf[slot, 2 * pol + 1, start : start + chunk]],
                    axis=1,
                ),
                weight[pol],
                preferred_element_type=jnp.float32,
            )
            for m in range(per_chunk):
                at = (start // SHORT + m) * PITCH
                left[at : at + SHORT] = part[m * SHORT : (m + 1) * SHORT, :LANES]
                right[at : at + SHORT] = part[m * SHORT : (m + 1) * SHORT, LANES:]

    def combine(i, start):
        def rows_at(at):
            return pl.ds((start // SHORT + at // SHORT) * PITCH + at % SHORT, per_chunk, stride=PITCH)

        def both(at):
            low, high = rows_at(at), rows_at(at + 2)
            return g00[low, :] + g01[high, :], g10[low, :] + g11[high, :]

        here = both(0)
        where = pl.ds(pl.multiple_of(core * count + start // SHORT, per_chunk), per_chunk)
        for at in range(SHORT):
            later = both(at + 1)
            value = jnp.where(
                first_pol,
                here[0] + pltpu.roll(later[0], LANES - SLOTS, 1),
                here[1] + pltpu.roll(later[1], SLOTS, 1),
            )
            spec[i, at, where, :] = value.astype(jnp.bfloat16)
            here = later

    def patch(i):
        where = pl.ds(pl.multiple_of(core * count + count - per_chunk, per_chunk), per_chunk)
        rows8 = came_edge[pl.ds(pl.multiple_of(beam_of(i) * HALO_ROWS, HALO_ROWS), HALO_ROWS), :]
        final = lax.broadcasted_iota(jnp.int32, (per_chunk, LANES), 0) == per_chunk - 1
        for n in range(TAPS - 1):
            at = SHORT - TAPS + 1 + n
            more = jnp.where(final, jnp.broadcast_to(rows8[n : n + 1], (per_chunk, LANES)), 0.0)
            spec[i, at, where, :] = (spec[i, at, where, :].astype(jnp.float32) + more).astype(jnp.bfloat16)

    def swap(i):
        half = pl.ds(pl.multiple_of(core * count, count), count)
        return pltpu.make_async_remote_copy(
            src_ref=spec.at[i, :, half, :],
            dst_ref=spec.at[i + 1, :, half, :],
            send_sem=swap_sent.at[i // 2],
            recv_sem=swap_came.at[i // 2],
            device_id=(tm, chan + 1 - 2 * core),
            device_id_type=MESH,
        )

    def fine_first(i):
        sign_full = sign_of(LANES).astype(jnp.bfloat16)
        for at in range(SHORT):
            plain = spec[i, at]
            flipped = pltpu.roll(plain, LANES // 2, 1) * sign_full
            mid[at, :LANES] = jnp.dot(
                dft[at],
                jnp.concatenate(
                    [jnp.concatenate([plain, flipped], axis=0), jnp.concatenate([flipped, -plain], axis=0)], axis=1
                ),
                preferred_element_type=jnp.float32,
            )

    def fine_second(at_row):
        rows8 = pl.ds(at_row, 8)
        spectra = short_dft([(mid[at, rows8, :LANES], mid[at, rows8, LANES:]) for at in range(SHORT)], True)
        for high, value in enumerate(spectra):
            where = pl.ds(high // 2 * LANES + at_row, 8)
            power[where, high % 2 * LANES : (high % 2 + 1) * LANES] = (value * value).astype(jnp.bfloat16)

    def fine_last(item):
        for pair in range(FINE // BLOCK // 2):
            sums = lax.dot_general(
                pick_ref[...],
                power[pair * BLOCK : (pair + 1) * BLOCK, :],
                (((1,), (1,)), ((), ())),
                preferred_element_type=jnp.float32,
            )
            for group in range(chan_devices):
                for side in range(2):
                    send[item, group, 2 * pair + side] = sums[
                        group * 8 : group * 8 + 8, side * LANES : (side + 1) * LANES
                    ].astype(jnp.bfloat16)

    def along_chan(item, k):
        return pltpu.make_async_remote_copy(
            src_ref=send.at[item, chan_peers[k]],
            dst_ref=held.at[item, k],
            send_sem=sent1.at[item, k],
            recv_sem=came1.at[item, k],
            device_id=(tm, chan_peers[k]),
            device_id_type=MESH,
        )

    def along_tm(item, k, q):
        block = held.at[item, k] if k else send.at[item, chan]
        return pltpu.make_async_remote_copy(
            src_ref=block.at[pl.ds(first_block(tm_peers[q]), 4)],
            dst_ref=out_ref.at[tm, chan_peers[k], item],
            send_sem=sent2.at[item, k, q],
            recv_sem=came2.at[item, k, q],
            device_id=(tm_peers[q], chan),
            device_id_type=MESH,
        )

    def near_copy(item, k):
        block = held.at[item, k] if k else send.at[item, chan]
        return pltpu.make_async_copy(
            block.at[pl.ds(first_block(tm), 4)], out_ref.at[tm, chan_peers[k], item], near_sem.at[item, k]
        )

    def forward(item):
        for k in range(chan_devices):
            if k:
                along_chan(item, k).wait_recv()
            for q in range(tm_count - 1, 0, -1):
                along_tm(item, k, q).start()
            near_copy(item, k).start()

    def coarse_start(i):
        volt_copy(i).wait()

        @pl.when(i + 2 < beams)
        def _():
            volt_copy(i + 2).start()

    def coarse_rest(i):
        for start in range(chunk, rows, chunk):
            matmuls(lax.rem(i, DEPTH), start)
            combine(i, start - chunk)

    def share(item):
        for k in far_first:
            along_chan(item, k).start()

        @pl.when(item > 0)
        def _():
            forward(item - 1)

    @pl.loop(0, items)
    def _(pair):
        i = 2 * pair
        done = jnp.maximum(i - 1, 0)
        item = jnp.maximum(pair - 1, 0)
        coarse_start(i)
        matmuls(lax.rem(i, DEPTH), 0)
        combine(done, rows - chunk)

        @pl.when(pair == 0)
        def _():
            coarse_rest(i)

        @pl.when(pair > 0)
        def _():
            @pl.when(pair == 1)
            def _():
                dft_copy.wait()

            patch(i - 1)
            swap(i - 2).wait_recv()
            fine_first(done)
            groups = list(range(0, LANES, 8))
            for start in range(chunk, rows, chunk):
                matmuls(lax.rem(i, DEPTH), start)
                combine(i, start - chunk)
                share_of = len(groups) // ((rows - start) // chunk)
                for at_row in groups[:share_of]:
                    fine_second(at_row)
                groups = groups[share_of:]
            fine_last(item)
            share(item)

        coarse_start(i + 1)
        matmuls(lax.rem(i + 1, DEPTH), 0)
        combine(i, rows - chunk)

        @pl.when(pair == 0)
        def _():
            @pl.when(place < last_place)
            def _():
                edge_copy.wait_recv()

            @pl.when(place == last_place)
            def _():
                came_edge[...] = jnp.zeros_like(came_edge)

        patch(i)
        swap(i).start()
        coarse_rest(i + 1)

    combine(beams - 1, rows - chunk)
    patch(beams - 1)
    swap(beams - 2).wait_recv()
    fine_first(beams - 1)

    for at_row in range(0, LANES, 8):
        fine_second(at_row)
    fine_last(items - 1)
    share(items - 1)
    forward(items - 1)

    low_copy.wait()

    @pl.when(place > 0)
    def _():
        edge_copy.wait_send()

    @pl.loop(0, items)
    def _(item):
        swap(2 * item).wait_send()
        for k in range(chan_devices):
            if k:
                along_chan(item, k).wait_send()
            for q in range(1, tm_count):
                along_tm(item, k, q).wait_send()
            near_copy(item, k).wait()
        for k in range(chan_devices):
            for q in range(1, tm_count):
                pltpu.make_async_remote_copy(
                    src_ref=held.at[item, k, pl.ds(0, 4)],
                    dst_ref=out_ref.at[tm_peers[q], chan_peers[k], item],
                    send_sem=sent2.at[item, k, q],
                    recv_sem=came2.at[item, k, q],
                    device_id=(tm_peers[q], chan),
                    device_id_type=MESH,
                ).wait_recv()


def front(voltages, taps, busy_mask, drift_low, tm_count, chan_devices):
    beams, lanes, rows, chan_count = voltages.shape
    items = beams // 2
    ids = np.arange(chan_count)
    angles = (ids[:, None] * ids[None, :] % chan_count) * (2.0 * math.pi / chan_count)
    trig = jnp.asarray(np.stack([np.cos(angles), np.sin(angles)]), jnp.bfloat16)
    position = np.arange(SHORT)[:, None, None] + SHORT * np.arange(LANES)[None, None, :]
    turns = (position * np.arange(LANES)[None, :, None] % FINE) * (2.0 * math.pi / FINE)
    dft = jnp.asarray(np.concatenate([np.cos(turns), np.sin(turns)], axis=2), jnp.bfloat16)
    column = np.arange(2 * LANES)
    tap_of = np.stack([2 * (column // LANES) + (column // SLOTS % 2 ^ pol) for pol in range(2)])
    tap_pick = tap_of[:, None, :] == (np.arange(2 * TAPS) % TAPS)[None, :, None]
    per_group = SLOTS // chan_devices
    line = np.arange(8 * chan_devices)
    group, side, slot = line // 8, line % 8 // per_group, line % per_group
    lane = np.arange(2 * LANES)
    pick = (side[:, None] == lane[None, :] // LANES) & (
        (group * per_group + slot)[:, None] == lane[None, :] % SLOTS
    )
    hbm = pl.BlockSpec(memory_space=pl.ANY)
    dma = pltpu.SemaphoreType.DMA
    kernel = lambda *refs: front_kernel(tm_count, chan_devices, *refs)
    blocks = FINE // BLOCK
    gram = pltpu.VMEM(((rows // SHORT + 1) * PITCH, LANES), jnp.float32)
    return pl.pallas_call(
        kernel,
        in_specs=[hbm] * 8,
        out_specs=(hbm, hbm),
        out_shape=(
            jax.ShapeDtypeStruct((tm_count, chan_devices, items, 4, 8, LANES), jnp.bfloat16),
            jax.ShapeDtypeStruct((8, LANES), jnp.float32),
        ),
        scratch_shapes=[
            pltpu.VMEM(taps.shape, jnp.float32),
            pltpu.VMEM((1, chan_count), jnp.int32),
            pltpu.VMEM((1, chan_count), jnp.int32),
            pltpu.VMEM(tap_pick.shape, jnp.bfloat16),
            pltpu.VMEM(pick.shape, jnp.bfloat16),
            pltpu.VMEM((8, LANES), jnp.float32),
            pltpu.VMEM((DEPTH, lanes, rows, chan_count), jnp.bfloat16),
            pltpu.VMEM((beams, lanes, HALO_ROWS, chan_count), jnp.bfloat16),
            pltpu.VMEM(trig.shape, jnp.bfloat16),
            pltpu.VMEM(dft.shape, jnp.bfloat16),
            pltpu.VMEM((2, 2 * chan_count, 2 * LANES), jnp.bfloat16),
            pltpu.VMEM((beams * HALO_ROWS, LANES), jnp.float32),
            pltpu.VMEM((beams * HALO_ROWS, LANES), jnp.float32),
            gram,
            gram,
            gram,
            gram,
            pltpu.VMEM((beams, SHORT, LANES, LANES), jnp.bfloat16),
            pltpu.VMEM((SHORT, LANES + 8, 2 * LANES), jnp.float32),
            pltpu.VMEM((FINE // 2, 2 * LANES), jnp.bfloat16),
            pltpu.VMEM((items, chan_devices, blocks, 8, LANES), jnp.bfloat16),
            pltpu.VMEM((items, chan_devices, blocks, 8, LANES), jnp.bfloat16),
            dma((DEPTH,)),
            dma((3,)),
            dma((5,)),
            dma((2,)),
            dma((items,)),
            dma((items,)),
            dma((items, chan_devices)),
            dma((items, chan_devices)),
            dma((items, chan_devices, tm_count)),
            dma((items, chan_devices, tm_count)),
            dma((items, chan_devices)),
        ],
        compiler_params=pltpu.CompilerParams(
            collective_id=0, has_side_effects=True, vmem_limit_bytes=56 * 2**20
        ),
    )(
        voltages,
        taps,
        busy_mask.reshape(1, chan_count),
        drift_low.reshape(1, chan_count),
        trig,
        dft,
        jnp.asarray(tap_pick, jnp.bfloat16),
        jnp.asarray(pick, jnp.bfloat16),
    )


STRIDE = 40


def drift_kernel(scale, low_hbm, in_hbm, out_ref, low_ref, in_ref, rows_ref, stage_ref, sems):
    steps, beams, tiles, _, _ = in_ref.shape
    _, _, rates, width = out_ref.shape
    slots = rows_ref.shape[0]
    pad = PAD // LANES
    wide = 2 * tiles
    slot = pl.program_id(0)
    tm, chan = lax.axis_index("tm"), lax.axis_index("chan")
    parts = 4
    portion = steps // parts

    def arrival(n):
        span = pl.ds(n * portion, portion)
        return pltpu.make_async_copy(in_hbm.at[span], in_ref.at[span], sems.at[n])

    @pl.when(slot == 0)
    def _():
        low_copy = pltpu.make_async_copy(low_hbm, low_ref, sems.at[parts])
        for n in range(parts):
            arrival(n).start()
        low_copy.start()
        empty = jnp.zeros((beams, LANES), jnp.float32)

        @pl.loop(0, parts)
        def _(n):
            arrival(n).wait()

            for step in range(portion):
                t = n * portion + step
                for beam in range(beams):
                    stage_ref[step, beam * STRIDE : beam * STRIDE + 8 * tiles] = (
                        in_ref[t, beam].astype(jnp.float32).reshape(8 * tiles, LANES)
                    )
                for at in range(slots):
                    rows = [empty] * pad
                    rows += [stage_ref[step, pl.ds(tile * slots + at, beams, stride=STRIDE), :] for tile in range(wide)]
                    rows += [empty] * pad
                    for tile in range(wide + 2 * pad - 2):
                        rows_ref[at, t, tile] = jnp.concatenate([rows[tile], rows[tile + 2]], axis=0).astype(
                            jnp.bfloat16
                        )

        low_copy.wait()

    lane8 = lax.broadcasted_iota(jnp.int32, (8, LANES), 1)
    low = jnp.sum(jnp.where(lane8 == chan * slots + slot, low_ref[...], 0.0)[:1]).astype(jnp.int32)
    lane = lax.broadcasted_iota(jnp.int32, (2 * beams, LANES), 1)
    origin = tm * width - BLOCK * first_block(tm) + PAD
    for rate in range(rates):
        totals = None
        for t in range(steps):
            start = (low * t + origin) + rate * t
            base = lax.shift_right_logical(start, 7)
            if t:
                rest = start & (LANES - 1)
                back = (LANES - rest) & (LANES - 1)
                keep = lane >= rest
                three = rows_ref[slot, t, pl.ds(base, 3)]
                even, odd = [
                    pltpu.roll(jnp.where(keep, three[k], three[k + 1]), back, 1).astype(jnp.float32) for k in range(2)
                ]
            else:
                two = rows_ref[slot, t, pl.ds(base, 2)]
                even, odd = two[0].astype(jnp.float32), two[1].astype(jnp.float32)
            added = [even[:beams], odd[:beams], even[beams:], odd[beams:]]
            totals = added if totals is None else [total + more for total, more in zip(totals, added)]
        out_ref[:, 0, rate, :] = jnp.concatenate(totals, axis=1) * scale


def drift_sums(arrived, low_rates, slots, width):
    steps, beams, tiles, _, _ = arrived.shape
    kernel = lambda *refs: drift_kernel(1.0 / (4.0 * FINE * steps), *refs)
    hbm = pl.BlockSpec(memory_space=pl.ANY)
    return pl.pallas_call(
        kernel,
        grid=(slots,),
        in_specs=[hbm, hbm],
        out_specs=pl.BlockSpec((beams, 1, NDRIFT, width), lambda s: (0, s, 0, 0)),
        out_shape=jax.ShapeDtypeStruct((beams, slots, NDRIFT, width), jnp.float32),
        scratch_shapes=[
            pltpu.VMEM((8, LANES), jnp.float32),
            pltpu.VMEM(arrived.shape, jnp.bfloat16),
            pltpu.VMEM((slots, steps, 2 * tiles + 2 * PAD // LANES - 2, 2 * beams, LANES), jnp.bfloat16),
            pltpu.VMEM((steps // 4, beams * STRIDE, LANES), jnp.float32),
            pltpu.SemaphoreType.DMA((5,)),
        ],
        compiler_params=pltpu.CompilerParams(vmem_limit_bytes=60 * 2**20),
    )(low_rates, arrived)


def paired_shards(voltages, taps, busy_mask, drift_low):
    tm_count = lax.axis_size("tm")
    chan_devices = lax.axis_size("chan")
    arrived, low_rates = front(voltages, taps, busy_mask, drift_low, tm_count, chan_devices)
    arrived = arrived.reshape(tm_count * chan_devices // 2, voltages.shape[0], 4, 8, LANES)
    return drift_sums(arrived, low_rates, SLOTS // chan_devices, FINE // tm_count)


def two_devices_hold_a_step(mesh, voltages):
    tm_count, chan_devices = mesh.shape["tm"], mesh.shape["chan"]
    rows = voltages.shape[2] // (tm_count * chan_devices)
    return (
        2 * rows == FINE
        and tm_count == 4
        and chan_devices == 2 * FSTEP
        and CH_DEV * tm_count * chan_devices == SLOTS
        and voltages.shape[0] == 8
        and PAD >= DSPAN * (FSTEP * tm_count - 1)
    )


def solution(mesh):
    in_specs = (P(None, None, ("tm", "chan"), None), P(), P(), P())
    out_specs = P(None, "chan", None, "tm")

    def run(voltages, taps, busy_mask, drift_low):
        body = paired_shards if two_devices_hold_a_step(mesh, voltages) else shards
        return jax.shard_map(
            body, mesh=mesh, in_specs=in_specs, out_specs=out_specs, check_vma=False
        )(voltages, taps, busy_mask, drift_low)

    return run
```
